256 devices in a mesh: fft: 32 (over z, x_lo, core), band: 8 (over y, x_hi).
Axes of the slice: x: 4 (x_hi: 2, x_lo: 2; x = x_hi * 2 + x_lo), y: 4, z: 8, core: 2. Of those that a mesh axis runs over, the one named last changes fastest.
Arguments:
- wavefunctions: float32 [2, 16, 128, 128, 128], P(None, 'band', 'fft'), may hold values from -6 to 6
- potential: float32 [128, 128, 128], P('fft'), may hold values from -30 to 10
- occupation: float32 [16], P('band'), may hold values from 0.0125 to 0.25
Outputs:
- propagated: float32 [2, 16, 128, 128, 128], P(None, 'band', 'fft')
- reduced_gradient: float32 [128, 128, 128], P('fft', 'band')
- exchange_density: float32 [128, 128, 128], P('fft', 'band')
The draws below stay inside these ranges and needn't reach their ends.
All inputs are finite; a program needn't handle non-finite values.
Results may differ from the reference program's by a relative error of at most 0.0003.
Values sent between devices are 32-bit elements; how exact they have to be, the bound alone decides.
A program may use at most 64 MiB of HBM per device.

```python
import math
import jax
import jax.numpy as jnp
from jax import lax

GRID = 128
BANDS = 16


def draw_wavefunctions(key, part):
    shape_envelope = (2, BANDS, 1, GRID, GRID)
    shape_whole = (2, BANDS, GRID, GRID, GRID)
    planes = jnp.arange(GRID, dtype=jnp.int32)
    alternate = (1 - 2 * (planes % 2)).astype(jnp.float32)[None, None, :, None, None]
    phase_angle = planes.astype(jnp.float32) * (2.0 * math.pi / GRID)
    cosine = jnp.cos(phase_angle)[None, None, :, None, None]
    sine_wave = jnp.sin(phase_angle)[None, None, :, None, None]
    first_key = jax.random.fold_in(key, 11)
    second_key = jax.random.fold_in(key, 12)
    third_key = jax.random.fold_in(key, 13)
    fourth_key = jax.random.fold_in(key, 14)
    offset_part = 0.7 * jax.random.normal(first_key, shape_envelope, jnp.float32)
    swing_cos = 0.7 * jax.random.normal(second_key, shape_envelope, jnp.float32)
    swing_sin = 0.7 * jax.random.normal(third_key, shape_envelope, jnp.float32)
    rough_part = 0.35 * jax.random.normal(fourth_key, shape_whole, jnp.float32)
    envelope = offset_part + swing_cos * cosine + swing_sin * sine_wave
    values = alternate * envelope + rough_part
    return jnp.clip(values, -6.0, 6.0).astype(jnp.float32)


def draw_potential(key, part):
    side_key = jax.random.fold_in(key, 31)
    depth_key = jax.random.fold_in(key, 32)
    chosen = jax.random.bernoulli(side_key, 0.5, (GRID, GRID, GRID))
    sides = jnp.where(chosen, 1.0, -1.0).astype(jnp.float32)
    spread = jax.random.uniform(depth_key, (GRID, GRID, GRID), jnp.float32, 0.0, 1.0)
    depth = 0.6 + 0.4 * spread
    return (-10.0 + 20.0 * sides * depth).astype(jnp.float32)


def shard_levels(stream_key, shape, split, low, largest):
    def one(dim, blocks):
        heights = jax.random.uniform(jax.random.fold_in(jax.random.fold_in(stream_key, 6), dim), (blocks,), jnp.float32, low / len(split), largest / len(split))
        return jnp.repeat(jnp.exp(heights), shape[dim] // blocks).reshape((-1,) + (1,) * (len(shape) - dim - 1))

    gain = one(*split[0])
    for cut in split[1:]:
        gain = gain * one(*cut)
    return gain


def setup_inputs(seed: int = 0) -> dict:
    key_of = jax.random.split(jax.random.key(seed), 4)
    wavefunctions = draw_wavefunctions(jax.random.fold_in(key_of[3], 71), 0)
    potential = draw_potential(jax.random.fold_in(key_of[3], 71), 0)
    occupation = jnp.clip(jnp.exp(math.log(0.25) - 2.9957323 * jax.random.uniform(key_of[2], (BANDS,), jnp.float32) ** shard_levels(key_of[2], (BANDS,), ((0, 8),), -0.2, 0.2)), 0.0125, 0.25)
    return dict(wavefunctions=wavefunctions, potential=potential, occupation=occupation)


SPACING = 0.4
TIME_STEP = 0.012
KAPPA_PBE = 0.804
MU_PBE = 0.21951
FERMI_FACTOR = 2.0 * math.pow(3.0 * math.pi * math.pi, 1.0 / 3.0)
SLATER_FACTOR = 0.75 * math.pow(3.0 / math.pi, 1.0 / 3.0)

def kinetic_grid():
    wavenumber = jnp.fft.fftfreq(GRID) * (2.0 * math.pi / SPACING)
    squared = wavenumber * wavenumber
    return 0.5 * (squared[:, None, None] + squared[None, :, None] + squared[None, None, :])

def hamiltonian(field, potential, kinetic):
    return jnp.fft.ifftn(kinetic * jnp.fft.fftn(field)) + potential * field

def periodic_derivative(values, dimension):
    nearer = jnp.roll(values, -1, dimension) - jnp.roll(values, 1, dimension)
    farther = jnp.roll(values, -2, dimension) - jnp.roll(values, 2, dimension)
    return (8.0 * nearer - farther) / (12.0 * SPACING)

def exchange_terms(density, grad_z, grad_x, grad_y):
    gradient_norm = jnp.sqrt(grad_z * grad_z + grad_x * grad_x + grad_y * grad_y)
    power = jnp.power(density, 4.0 / 3.0)
    reduced = gradient_norm / (FERMI_FACTOR * power)
    enhance = 1.0 + KAPPA_PBE - KAPPA_PBE / (1.0 + MU_PBE * reduced * reduced / KAPPA_PBE)
    return (reduced, -SLATER_FACTOR * power * enhance)

def reference(wavefunctions, potential, occupation):
    kinetic = kinetic_grid()

    def one_band(density, inputs):
        real_part, imag_part, weight = inputs
        field = real_part + 1j * imag_part
        first = hamiltonian(field, potential, kinetic)
        second = hamiltonian(first, potential, kinetic)
        result = field - 1j * TIME_STEP * first - 0.5 * TIME_STEP * TIME_STEP * second
        new_real = jnp.real(result)
        new_imag = jnp.imag(result)
        density = density + weight * (new_real * new_real + new_imag * new_imag)
        return (density, (new_real, new_imag))
    start_density = jnp.zeros(potential.shape, jnp.float32)
    density, outputs = lax.scan(one_band, start_density, (wavefunctions[0], wavefunctions[1], occupation))
    propagated = jnp.stack([outputs[0], outputs[1]])
    grad_z = periodic_derivative(density, 0)
    grad_x = periodic_derivative(density, 1)
    grad_y = periodic_derivative(density, 2)
    reduced, energy = exchange_terms(density, grad_z, grad_x, grad_y)
    return (propagated, reduced, energy)
```

```python
import functools
import math

import jax
import jax.numpy as jnp
import numpy as np
from jax import lax
from jax.experimental import pallas as pl
from jax.experimental.pallas import tpu as pltpu
from jax.sharding import PartitionSpec as P

SPACING = 0.4
TIME_STEP = 0.012
HALF_SQUARE = 0.5 * TIME_STEP * TIME_STEP
KAPPA_PBE = 0.804
MU_PBE = 0.21951
FERMI_FACTOR = 2.0 * math.pow(3.0 * math.pi * math.pi, 1.0 / 3.0)
SLATER_FACTOR = 0.75 * math.pow(3.0 / math.pi, 1.0 / 3.0)

GRID = 128
FFT = 32
BAND = 8
PLANES = GRID // FFT
ROWS = 8
OWN_ROWS = GRID // BAND
MESH = pl.DeviceIdType.MESH
F32 = jnp.float32
BF16 = jnp.bfloat16


def kinetic_matrix():
    counter = np.arange(GRID)
    signed = np.where(counter < GRID // 2, counter, counter - GRID)
    half_squares = 0.5 * (2.0 * np.pi * signed / (GRID * SPACING)) ** 2
    phase = np.outer(counter, counter) % GRID
    column = np.cos(2.0 * np.pi * phase / GRID) @ half_squares / GRID
    return column[(counter[:, None] - counter[None, :]) % GRID]


def kinetic_parts():
    matrix = kinetic_matrix()
    high = matrix.astype(jnp.bfloat16)
    low = (matrix - high.astype(np.float64)).astype(jnp.bfloat16)
    return np.stack([high, low])


def split(values):
    high = values.astype(BF16)
    return high, (values - high.astype(F32)).astype(BF16)


def dot(a, b):
    return jnp.dot(a, b, preferred_element_type=F32)


def from_left(table, values):
    high, low = split(values)
    return dot(table[0], high) + dot(table[0], low) + dot(table[1], high)


def in_plane(table, values):
    high, low = split(values)
    left = dot(table[0], high) + dot(table[0], low) + dot(table[1], high)
    right = dot(high, table[0]) + dot(low, table[0]) + dot(high, table[1])
    return left + right


def wait_bytes(ref, sem):
    pltpu.make_async_copy(ref, ref, sem).wait()


def kernel(
    occ,
    psi_hbm,
    pot_hbm,
    table_hbm,
    out_hbm,
    reduced_ref,
    energy_ref,
    psi,
    pot,
    table,
    tang,
    local,
    col,
    col_pot,
    back,
    ret,
    part,
    arrived,
    dens,
    halo_z,
    edge_x,
    halo_x,
    rows_x,
    sem_in,
    sem_out,
    sem_col,
    sem_tang,
    sem_ret,
    sem_group,
    sem_pot,
    sem_dens,
    sem_halo,
    send,
):
    me = lax.axis_index("fft")
    my_band = lax.axis_index("band")
    my_slot = me // 2
    my_chip = me // 4

    def fft_peer(step):
        k = (step + 1) // 2
        sign = 2 * (step % 2) - 1
        return lax.rem(me + sign * k + FFT, FFT)

    def rows_of(slot):
        return pl.ds(pl.multiple_of(slot * ROWS, ROWS), ROWS)

    def planes_of(device):
        return pl.ds(device * PLANES, PLANES)

    barrier = pltpu.get_barrier_semaphore()
    load_psi = pltpu.make_async_copy(psi_hbm, psi, sem_in.at[0])
    load_pot = pltpu.make_async_copy(pot_hbm, pot, sem_in.at[1])
    load_table = pltpu.make_async_copy(table_hbm, table, sem_in.at[2])
    load_psi.start()
    load_pot.start()
    load_table.start()

    @pl.loop(1, FFT)
    def _(step):
        pl.semaphore_signal(
            barrier, inc=1, device_id={"fft": fft_peer(step)}, device_id_type=MESH
        )

    @pl.loop(1, BAND)
    def _(step):
        pl.semaphore_signal(
            barrier,
            inc=1,
            device_id={"band": lax.rem(my_band + step, BAND)},
            device_id_type=MESH,
        )

    load_psi.wait()
    load_pot.wait()
    load_table.wait()
    pl.semaphore_wait(barrier, FFT + BAND - 2)

    @pl.loop(1, FFT)
    def _(step):
        peer = fft_peer(step)
        pltpu.make_async_remote_copy(
            src_ref=psi.at[:, peer % 2, :, rows_of(peer // 2), :],
            dst_ref=col.at[pl.ds(0, 2), planes_of(me)],
            send_sem=send.at[0],
            recv_sem=sem_col,
            device_id={"fft": peer},
            device_id_type=MESH,
        ).start()

    pltpu.make_async_copy(
        psi.at[:, me % 2, :, rows_of(my_slot), :],
        col.at[pl.ds(0, 2), planes_of(me)],
        sem_col,
    ).start()

    first_slot = lax.rem(my_band - me + FFT, BAND)
    for k in range(4):
        target = 2 * (first_slot + BAND * (k // 2)) + k % 2

        @pl.when(target != me)
        def _():
            pltpu.make_async_remote_copy(
                src_ref=pot.at[:, rows_of(target // 2), :],
                dst_ref=col_pot.at[planes_of(me)],
                send_sem=send.at[1],
                recv_sem=sem_pot.at[0],
                device_id={"fft": target},
                device_id_type=MESH,
            ).start()

        @pl.when(target == me)
        def _():
            pltpu.make_async_copy(
                pot.at[:, rows_of(my_slot), :],
                col_pot.at[planes_of(me)],
                sem_pot.at[0],
            ).start()

    kin = (table[0], table[1])

    for part_of in range(2):

        @pl.loop(0, 8)
        def _(index):
            band, plane = index // 4, index % 4
            tang[part_of, band, plane] = in_plane(kin, psi[part_of, band, plane])

        @pl.loop(1, FFT)
        def _(step):
            peer = fft_peer(step)
            pltpu.make_async_remote_copy(
                src_ref=tang.at[part_of, peer % 2, :, rows_of(peer // 2), :],
                dst_ref=col.at[2 + part_of, planes_of(me)],
                send_sem=send.at[2],
                recv_sem=sem_tang.at[part_of],
                device_id={"fft": peer},
                device_id_type=MESH,
            ).start()

        pltpu.make_async_copy(
            tang.at[part_of, me % 2, :, rows_of(my_slot), :],
            col.at[2 + part_of, planes_of(me)],
            sem_tang.at[part_of],
        ).start()

    wait_bytes(col_pot.at[pl.ds(0, 16)], sem_pot.at[0])
    first_device = lax.rem(my_band - my_slot + FFT, BAND)

    @pl.loop(0, 4)
    def _(k):
        held = planes_of(first_device + BAND * k)

        @pl.loop(1, BAND)
        def _(step):
            pltpu.make_async_remote_copy(
                src_ref=col_pot.at[held],
                dst_ref=col_pot.at[held],
                send_sem=send.at[3],
                recv_sem=sem_pot.at[1],
                device_id={"band": lax.rem(my_band + step, BAND)},
                device_id_type=MESH,
            ).start()

    @pl.loop(0, 8)
    def _(index):
        band, plane = index // 4, index % 4
        values = pot[plane]
        real, imag = psi[0, band, plane], psi[1, band, plane]
        first_real = tang[0, band, plane] + values * real
        first_imag = tang[1, band, plane] + values * imag
        second_real = in_plane(kin, first_real) + values * first_real
        second_imag = in_plane(kin, first_imag) + values * first_imag
        local[0, band, plane] = real + TIME_STEP * first_imag - HALF_SQUARE * second_real
        local[1, band, plane] = imag - TIME_STEP * first_real - HALF_SQUARE * second_imag

    wait_bytes(col.at[pl.ds(0, 2)], sem_col)
    wait_bytes(col_pot.at[pl.ds(0, 112)], sem_pot.at[1])
    for part_of in range(2):
        sign = 1.0 - 2.0 * part_of
        wait_bytes(col.at[2 + part_of], sem_tang.at[part_of])

        @pl.loop(0, ROWS)
        def _(row):
            values = col_pot[:, row, :]
            mine = col[part_of, :, row, :]
            other = col[1 - part_of, :, row, :]
            along = from_left(kin, mine)
            inner = (
                (sign * TIME_STEP) * other
                - (2.0 * HALF_SQUARE) * col[2 + part_of, :, row, :]
                - HALF_SQUARE * (values * mine + along)
            )
            back[part_of, :, row, :] = from_left(kin, inner) - HALF_SQUARE * (values * along)

        @pl.loop(1, FFT)
        def _(step):
            peer = fft_peer(step)
            pltpu.make_async_remote_copy(
                src_ref=back.at[part_of, planes_of(peer)],
                dst_ref=ret.at[part_of, me % 2, :, rows_of(my_slot), :],
                send_sem=send.at[4],
                recv_sem=sem_ret if part_of == 0 else sem_group.at[my_chip],
                device_id={"fft": peer},
                device_id_type=MESH,
            ).start()

        pltpu.make_async_copy(
            back.at[part_of, planes_of(me)],
            ret.at[part_of, me % 2, :, rows_of(my_slot), :],
            sem_ret if part_of == 0 else sem_group.at[my_chip],
        ).start()

    wait_bytes(ret.at[0], sem_ret)

    @pl.loop(0, PLANES)
    def _(plane):
        low = local[0, 0, plane] + ret[0, 0, plane]
        high = local[0, 1, plane] + ret[0, 1, plane]
        local[0, 0, plane] = low
        local[0, 1, plane] = high
        part[plane] = occ[0] * (low * low) + occ[1] * (high * high)

    store_real = pltpu.make_async_copy(local.at[0], out_hbm.at[0], sem_out.at[0])
    store_real.start()

    @pl.loop(0, BAND)
    def _(step):
        k = (step + 1) // 2
        sign = 2 * (step % 2) - 1
        block = lax.rem(my_chip + sign * k + BAND, BAND)
        rows = pl.ds(pl.multiple_of(block * OWN_ROWS, OWN_ROWS), OWN_ROWS)
        wait_bytes(ret.at[1, :, :, pl.ds(0, OWN_ROWS), :], sem_group.at[block])
        low = local[1, 0, :, rows, :] + ret[1, 0, :, rows, :]
        high = local[1, 1, :, rows, :] + ret[1, 1, :, rows, :]
        local[1, 0, :, rows, :] = low
        local[1, 1, :, rows, :] = high
        part[:, rows, :] = part[:, rows, :] + (occ[0] * (low * low) + occ[1] * (high * high))

        @pl.when(block != my_band)
        def _():
            pltpu.make_async_remote_copy(
                src_ref=part.at[:, rows, :],
                dst_ref=arrived.at[my_band],
                send_sem=send.at[5],
                recv_sem=sem_dens,
                device_id={"band": block},
                device_id_type=MESH,
            ).start()

        @pl.when(block == my_band)
        def _():
            pltpu.make_async_copy(part.at[:, rows, :], arrived.at[my_band], sem_dens).start()

    store_imag = pltpu.make_async_copy(local.at[1], out_hbm.at[1], sem_out.at[1])
    store_imag.start()

    wait_bytes(arrived, sem_dens)
    total = arrived[0]
    for k in range(1, BAND):
        total = total + arrived[k]
    dens[...] = total
    rows_x[:, 8:24, :] = total
    edge_x[0] = dens[:, 14:16, :]
    edge_x[1] = dens[:, 0:2, :]

    halos = []
    for side in range(2):
        shift = 1 - 2 * side
        halos.append(
            pltpu.make_async_remote_copy(
                src_ref=dens.at[pl.ds(2 - 2 * side, 2)],
                dst_ref=halo_z.at[side],
                send_sem=send.at[6 + side],
                recv_sem=sem_halo.at[side],
                device_id={"fft": lax.rem(me + shift + FFT, FFT)},
                device_id_type=MESH,
            )
        )
        halos.append(
            pltpu.make_async_remote_copy(
                src_ref=edge_x.at[side],
                dst_ref=halo_x.at[side],
                send_sem=send.at[8 + side],
                recv_sem=sem_halo.at[2 + side],
                device_id={"band": lax.rem(my_band + shift + BAND, BAND)},
                device_id_type=MESH,
            )
        )
    for halo in halos:
        halo.start()

    scale = 1.0 / (12.0 * SPACING)
    grad_y = (
        8.0 * (pltpu.roll(total, GRID - 1, 2) - pltpu.roll(total, 1, 2))
        - (pltpu.roll(total, GRID - 2, 2) - pltpu.roll(total, 2, 2))
    ) * scale
    power = jnp.exp((4.0 / 3.0) * jnp.log(total))

    wait_bytes(col.at[pl.ds(0, 2), pl.ds(0, 124)], send.at[0])
    wait_bytes(col.at[pl.ds(0, 2), pl.ds(0, 124)], send.at[2])
    wait_bytes(back.at[:, pl.ds(0, 124)], send.at[4])
    wait_bytes(col_pot.at[pl.ds(0, 112)], send.at[3])
    wait_bytes(arrived.at[pl.ds(0, 7)], send.at[5])
    holds_own = lax.rem(me + my_slot - my_band + FFT, BAND) == 0

    @pl.when(holds_own)
    def _():
        wait_bytes(col_pot.at[pl.ds(0, 12)], send.at[1])

    @pl.when(jnp.logical_not(holds_own))
    def _():
        wait_bytes(col_pot.at[pl.ds(0, 16)], send.at[1])

    for halo in halos:
        halo.wait()
    rows_x[:, 6:8, :] = halo_x[0]
    rows_x[:, 24:26, :] = halo_x[1]
    grad_x = (
        8.0 * (rows_x[:, 9:25, :] - rows_x[:, 7:23, :])
        - (rows_x[:, 10:26, :] - rows_x[:, 6:22, :])
    ) * scale
    stack = jnp.concatenate([halo_z[0], total, halo_z[1]], axis=0)
    grad_z = (8.0 * (stack[3:7] - stack[1:5]) - (stack[4:8] - stack[0:4])) * scale
    norm = jnp.sqrt(grad_z * grad_z + grad_x * grad_x + grad_y * grad_y)
    reduced = norm / (FERMI_FACTOR * power)
    enhance = 1.0 + KAPPA_PBE - KAPPA_PBE / (1.0 + MU_PBE * reduced * reduced / KAPPA_PBE)
    reduced_ref[...] = reduced
    energy_ref[...] = -SLATER_FACTOR * power * enhance
    store_real.wait()
    store_imag.wait()


def per_device(wavefunctions, potential, occupation):
    any_space = pl.BlockSpec(memory_space=pl.ANY)
    vmem = pl.BlockSpec(memory_space=pltpu.VMEM)
    block = (PLANES, OWN_ROWS, GRID)
    planes = (2, 2, PLANES, GRID, GRID)
    dma = pltpu.SemaphoreType.DMA
    return pl.pallas_call(
        kernel,
        name="taylor_step",
        out_shape=(
            jax.ShapeDtypeStruct(planes, F32),
            jax.ShapeDtypeStruct(block, F32),
            jax.ShapeDtypeStruct(block, F32),
        ),
        in_specs=[pl.BlockSpec(memory_space=pltpu.SMEM), any_space, any_space, any_space],
        out_specs=(any_space, vmem, vmem),
        scratch_shapes=[
            pltpu.VMEM(planes, F32),
            pltpu.VMEM((PLANES, GRID, GRID), F32),
            pltpu.VMEM((2, GRID, GRID), BF16),
            pltpu.VMEM(planes, F32),
            pltpu.VMEM(planes, F32),
            pltpu.VMEM((4, GRID, ROWS, GRID), F32),
            pltpu.VMEM((GRID, ROWS, GRID), F32),
            pltpu.VMEM((2, GRID, ROWS, GRID), F32),
            pltpu.VMEM(planes, F32),
            pltpu.VMEM((PLANES, GRID, GRID), F32),
            pltpu.VMEM((BAND, *block), F32),
            pltpu.VMEM(block, F32),
            pltpu.VMEM((2, 2, OWN_ROWS, GRID), F32),
            pltpu.VMEM((2, PLANES, 2, GRID), F32),
            pltpu.VMEM((2, PLANES, 2, GRID), F32),
            pltpu.VMEM((PLANES, 32, GRID), F32),
            dma((3,)),
            dma((2,)),
            dma,
            dma((2,)),
            dma,
            dma((BAND,)),
            dma((2,)),
            dma,
            dma((4,)),
            dma((10,)),
        ],
        compiler_params=pltpu.CompilerParams(
            collective_id=0, has_side_effects=True, vmem_limit_bytes=40 * 1024 * 1024
        ),
    )(occupation, wavefunctions, potential, kinetic_parts())


def solution(mesh):
    in_specs = (P(None, "band", "fft", None, None), P("fft", None, None), P("band"))
    out_specs = (P(None, "band", "fft", None, None), P("fft", "band", None), P("fft", "band", None))
    return jax.shard_map(
        per_device, mesh=mesh, in_specs=in_specs, out_specs=out_specs, check_vma=False
    )
```

```python
import functools
import math

import jax
import jax.numpy as jnp
import numpy as np
from jax import lax
from jax.experimental import pallas as pl
from jax.experimental.pallas import tpu as pltpu
from jax.sharding import PartitionSpec as P

SPACING = 0.4
TIME_STEP = 0.012
HALF_SQUARE = 0.5 * TIME_STEP * TIME_STEP
KAPPA_PBE = 0.804
MU_PBE = 0.21951
FERMI_FACTOR = 2.0 * math.pow(3.0 * math.pi * math.pi, 1.0 / 3.0)
SLATER_FACTOR = 0.75 * math.pow(3.0 / math.pi, 1.0 / 3.0)

GRID = 128
FFT = 32
BAND = 8
PLANES = GRID // FFT
ROWS = 8
OWN_ROWS = GRID // BAND
MESH = pl.DeviceIdType.MESH
F32 = jnp.float32
BF16 = jnp.bfloat16


def kinetic_matrix():
    counter = np.arange(GRID)
    signed = np.where(counter < GRID // 2, counter, counter - GRID)
    half_squares = 0.5 * (2.0 * np.pi * signed / (GRID * SPACING)) ** 2
    phase = np.outer(counter, counter) % GRID
    column = np.cos(2.0 * np.pi * phase / GRID) @ half_squares / GRID
    return column[(counter[:, None] - counter[None, :]) % GRID]


def kinetic_parts():
    matrix = kinetic_matrix()
    high = matrix.astype(jnp.bfloat16)
    low = (matrix - high.astype(np.float64)).astype(jnp.bfloat16)
    beside = np.concatenate([high, high, low], axis=1)
    return beside, beside.T.copy()


def split(values):
    high = values.astype(BF16)
    return high, (values - high.astype(F32)).astype(BF16)


def dot(a, b):
    return jnp.dot(a, b, preferred_element_type=F32)


def from_left(left, values):
    high, low = split(values)
    return dot(left, jnp.concatenate([high, low, high], axis=0))


def in_plane(left, right, values):
    high, low = split(values)
    return dot(left, jnp.concatenate([high, low, high], axis=0)) + dot(
        jnp.concatenate([high, low, high], axis=1), right
    )


def wait_bytes(ref, sem):
    pltpu.make_async_copy(ref, ref, sem).wait()


def kernel(
    occ_hbm,
    psi_hbm,
    pot_hbm,
    left_hbm,
    right_hbm,
    out_hbm,
    summed_ref,
    occ,
    psi,
    pot,
    left_table,
    right_table,
    tang,
    local,
    col,
    col_pot,
    back,
    ret,
    part,
    arrived,
    dens,
    halo_z,
    edge_x,
    halo_x,
    rows_x,
    sem_in,
    sem_out,
    sem_col,
    sem_tang,
    sem_ret,
    sem_group,
    sem_pot,
    sem_dens,
    sem_halo,
    send,
):
    me = lax.axis_index("fft")
    my_band = lax.axis_index("band")
    my_slot = me // 2
    my_chip = me // 4

    def fft_peer(step):
        k = (step + 1) // 2
        sign = 2 * (step % 2) - 1
        return lax.rem(me + sign * k + FFT, FFT)

    def rows_of(slot):
        return pl.ds(pl.multiple_of(slot * ROWS, ROWS), ROWS)

    def planes_of(device):
        return pl.ds(device * PLANES, PLANES)

    barrier = pltpu.get_barrier_semaphore()

    @pl.loop(1, FFT)
    def _(step):
        pl.semaphore_signal(
            barrier,
            inc=1,
            device_id={"fft": lax.rem(me + step, FFT)},
            device_id_type=MESH,
        )

    @pl.loop(1, BAND)
    def _(step):
        pl.semaphore_signal(
            barrier,
            inc=1,
            device_id={"band": lax.rem(my_band + step, BAND)},
            device_id_type=MESH,
        )

    loads = [
        pltpu.make_async_copy(source, target, sem_in.at[k])
        for k, (source, target) in enumerate((
            (psi_hbm, psi),
            (pot_hbm, pot),
            (left_hbm, left_table),
            (right_hbm, right_table),
            (occ_hbm, occ),
        ))
    ]
    for load in loads:
        load.start()
    for load in loads:
        load.wait()
    pl.semaphore_wait(barrier, FFT + BAND - 2)

    first_slot = lax.rem(my_band - me + FFT, BAND)
    for k in range(4):
        target = 2 * (first_slot + BAND * (k // 2)) + k % 2

        @pl.when(target != me)
        def _():
            pltpu.make_async_remote_copy(
                src_ref=pot.at[:, rows_of(target // 2), :],
                dst_ref=col_pot.at[planes_of(me)],
                send_sem=send.at[1],
                recv_sem=sem_pot.at[0],
                device_id={"fft": target},
                device_id_type=MESH,
            ).start()

        @pl.when(target == me)
        def _():
            pltpu.make_async_copy(
                pot.at[:, rows_of(my_slot), :],
                col_pot.at[planes_of(me)],
                sem_pot.at[0],
            ).start()

    @pl.loop(1, FFT)
    def _(step):
        peer = fft_peer(step)
        pltpu.make_async_remote_copy(
            src_ref=psi.at[:, peer % 2, :, rows_of(peer // 2), :],
            dst_ref=col.at[pl.ds(0, 2), planes_of(me)],
            send_sem=send.at[0],
            recv_sem=sem_col,
            device_id={"fft": peer},
            device_id_type=MESH,
        ).start()

    pltpu.make_async_copy(
        psi.at[:, me % 2, :, rows_of(my_slot), :],
        col.at[pl.ds(0, 2), planes_of(me)],
        sem_col,
    ).start()

    left, right = left_table[...], right_table[...]

    for part_of in range(2):

        @pl.loop(0, 8, unroll=4)
        def _(index):
            band, plane = index // 4, index % 4
            tang[part_of, band, plane] = in_plane(left, right, psi[part_of, band, plane])

        @pl.loop(1, FFT)
        def _(step):
            peer = fft_peer(step)
            pltpu.make_async_remote_copy(
                src_ref=tang.at[part_of, peer % 2, :, rows_of(peer // 2), :],
                dst_ref=col.at[2 + part_of, planes_of(me)],
                send_sem=send.at[2],
                recv_sem=sem_tang.at[part_of],
                device_id={"fft": peer},
                device_id_type=MESH,
            ).start()

        pltpu.make_async_copy(
            tang.at[part_of, me % 2, :, rows_of(my_slot), :],
            col.at[2 + part_of, planes_of(me)],
            sem_tang.at[part_of],
        ).start()

    wait_bytes(col_pot.at[pl.ds(0, 16)], sem_pot.at[0])
    first_device = lax.rem(my_band - my_slot + FFT, BAND)

    @pl.loop(0, 4)
    def _(k):
        held = planes_of(first_device + BAND * k)

        @pl.loop(1, BAND)
        def _(step):
            pltpu.make_async_remote_copy(
                src_ref=col_pot.at[held],
                dst_ref=col_pot.at[held],
                send_sem=send.at[3],
                recv_sem=sem_pot.at[1],
                device_id={"band": lax.rem(my_band + step, BAND)},
                device_id_type=MESH,
            ).start()

    @pl.loop(0, 8, unroll=2)
    def _(index):
        band, plane = index // 4, index % 4
        values = pot[plane]
        real, imag = psi[0, band, plane], psi[1, band, plane]
        first_real = tang[0, band, plane] + values * real
        first_imag = tang[1, band, plane] + values * imag
        second_real = in_plane(left, right, first_real) + values * first_real
        second_imag = in_plane(left, right, first_imag) + values * first_imag
        local[0, band, plane] = real + TIME_STEP * first_imag - HALF_SQUARE * second_real
        local[1, band, plane] = imag - TIME_STEP * first_real - HALF_SQUARE * second_imag

    wait_bytes(col.at[pl.ds(0, 2)], sem_col)
    wait_bytes(col_pot.at[pl.ds(0, 112)], sem_pot.at[1])
    for part_of in range(2):
        sign = 1.0 - 2.0 * part_of
        wait_bytes(col.at[2 + part_of], sem_tang.at[part_of])

        for pair in range(0, ROWS, 2):

            def rows(ref, *index):
                return jnp.concatenate(
                    [ref[(*index, slice(None), pair + k)] for k in range(2)], axis=1
                )

            values = rows(col_pot)
            mine = rows(col, part_of)
            along = from_left(left, mine)
            inner = (
                (sign * TIME_STEP) * rows(col, 1 - part_of)
                - (2.0 * HALF_SQUARE) * rows(col, 2 + part_of)
                - HALF_SQUARE * (values * mine + along)
            )
            moved = from_left(left, inner) - HALF_SQUARE * (values * along)
            for k in range(2):
                back[part_of, :, pair + k, :] = moved[:, k * GRID : (k + 1) * GRID]

        @pl.loop(1, FFT)
        def _(step):
            peer = fft_peer(step)
            pltpu.make_async_remote_copy(
                src_ref=back.at[part_of, planes_of(peer)],
                dst_ref=ret.at[part_of, me % 2, :, rows_of(my_slot), :],
                send_sem=send.at[4],
                recv_sem=sem_ret if part_of == 0 else sem_group.at[my_chip],
                device_id={"fft": peer},
                device_id_type=MESH,
            ).start()

        pltpu.make_async_copy(
            back.at[part_of, planes_of(me)],
            ret.at[part_of, me % 2, :, rows_of(my_slot), :],
            sem_ret if part_of == 0 else sem_group.at[my_chip],
        ).start()

    wait_bytes(ret.at[0], sem_ret)

    @pl.loop(0, PLANES)
    def _(plane):
        low = local[0, 0, plane] + ret[0, 0, plane]
        high = local[0, 1, plane] + ret[0, 1, plane]
        local[0, 0, plane] = low
        local[0, 1, plane] = high
        part[plane] = occ[0] * (low * low) + occ[1] * (high * high)

    store_real = pltpu.make_async_copy(local.at[0], out_hbm.at[0], sem_out.at[0])
    store_real.start()

    @pl.loop(0, BAND)
    def _(step):
        k = (step + 1) // 2
        sign = 2 * (step % 2) - 1
        block = lax.rem(my_chip + sign * k + BAND, BAND)
        rows = pl.ds(pl.multiple_of(block * OWN_ROWS, OWN_ROWS), OWN_ROWS)
        wait_bytes(ret.at[1, :, :, pl.ds(0, OWN_ROWS), :], sem_group.at[block])
        low = local[1, 0, :, rows, :] + ret[1, 0, :, rows, :]
        high = local[1, 1, :, rows, :] + ret[1, 1, :, rows, :]
        local[1, 0, :, rows, :] = low
        local[1, 1, :, rows, :] = high
        part[:, rows, :] = part[:, rows, :] + (occ[0] * (low * low) + occ[1] * (high * high))

        @pl.when(block != my_band)
        def _():
            pltpu.make_async_remote_copy(
                src_ref=part.at[:, rows, :],
                dst_ref=arrived.at[my_band],
                send_sem=send.at[5],
                recv_sem=sem_dens,
                device_id={"band": block},
                device_id_type=MESH,
            ).start()

        @pl.when(block == my_band)
        def _():
            pltpu.make_async_copy(part.at[:, rows, :], arrived.at[my_band], sem_dens).start()

    store_imag = pltpu.make_async_copy(local.at[1], out_hbm.at[1], sem_out.at[1])
    store_imag.start()

    wait_bytes(arrived, sem_dens)
    total = arrived[0]
    for k in range(1, BAND):
        total = total + arrived[k]
    dens[...] = total
    rows_x[:, 8:24, :] = total
    edge_x[0] = dens[:, 14:16, :]
    edge_x[1] = dens[:, 0:2, :]

    halos = []
    for side in range(2):
        shift = 1 - 2 * side
        halos.append(
            pltpu.make_async_remote_copy(
                src_ref=dens.at[pl.ds(2 - 2 * side, 2)],
                dst_ref=halo_z.at[side],
                send_sem=send.at[6 + side],
                recv_sem=sem_halo.at[side],
                device_id={"fft": lax.rem(me + shift + FFT, FFT)},
                device_id_type=MESH,
            )
        )
        halos.append(
            pltpu.make_async_remote_copy(
                src_ref=edge_x.at[side],
                dst_ref=halo_x.at[side],
                send_sem=send.at[8 + side],
                recv_sem=sem_halo.at[2 + side],
                device_id={"band": lax.rem(my_band + shift + BAND, BAND)},
                device_id_type=MESH,
            )
        )
    for halo in halos:
        halo.start()

    scale = 1.0 / (12.0 * SPACING)
    grad_y = (
        8.0 * (pltpu.roll(total, GRID - 1, 2) - pltpu.roll(total, 1, 2))
        - (pltpu.roll(total, GRID - 2, 2) - pltpu.roll(total, 2, 2))
    ) * scale

    wait_bytes(col.at[pl.ds(0, 2), pl.ds(0, 124)], send.at[0])
    wait_bytes(col.at[pl.ds(0, 2), pl.ds(0, 124)], send.at[2])
    wait_bytes(back.at[:, pl.ds(0, 124)], send.at[4])
    wait_bytes(col_pot.at[pl.ds(0, 112)], send.at[3])
    wait_bytes(arrived.at[pl.ds(0, 7)], send.at[5])
    holds_own = lax.rem(me + my_slot - my_band + FFT, BAND) == 0

    @pl.when(holds_own)
    def _():
        wait_bytes(col_pot.at[pl.ds(0, 12)], send.at[1])

    @pl.when(jnp.logical_not(holds_own))
    def _():
        wait_bytes(col_pot.at[pl.ds(0, 16)], send.at[1])

    for halo in halos:
        halo.wait()
    rows_x[:, 6:8, :] = halo_x[0]
    rows_x[:, 24:26, :] = halo_x[1]
    grad_x = (
        8.0 * (rows_x[:, 9:25, :] - rows_x[:, 7:23, :])
        - (rows_x[:, 10:26, :] - rows_x[:, 6:22, :])
    ) * scale
    stack = jnp.concatenate([halo_z[0], total, halo_z[1]], axis=0)
    grad_z = (8.0 * (stack[3:7] - stack[1:5]) - (stack[4:8] - stack[0:4])) * scale
    summed_ref[0] = grad_z * grad_z + grad_x * grad_x + grad_y * grad_y
    summed_ref[1] = total
    store_real.wait()
    store_imag.wait()


def exchange_terms(square, density):
    power = jnp.exp((4.0 / 3.0) * jnp.log(density))
    reduced = jnp.sqrt(square) / (FERMI_FACTOR * power)
    enhance = 1.0 + KAPPA_PBE - KAPPA_PBE / (1.0 + MU_PBE * reduced * reduced / KAPPA_PBE)
    return reduced, -SLATER_FACTOR * power * enhance


def finish(moved_in, summed_in, moved_out, reduced_out, energy_out, buffer, summed, terms, sem_in, sem_out):
    first = pltpu.make_async_copy(summed_in, summed, sem_in.at[4])
    first.start()
    loads = [
        pltpu.make_async_copy(moved_in.at[k // 2, k % 2], buffer.at[k], sem_in.at[k])
        for k in range(4)
    ]
    stores = [
        pltpu.make_async_copy(buffer.at[k], moved_out.at[k // 2, k % 2], sem_out.at[k])
        for k in range(4)
    ]
    stores.append(pltpu.make_async_copy(terms.at[0], reduced_out, sem_out.at[4]))
    stores.append(pltpu.make_async_copy(terms.at[1], energy_out, sem_out.at[5]))
    for load in loads:
        load.start()
    first.wait()
    terms[0], terms[1] = exchange_terms(summed[0], summed[1])
    stores[4].start()
    stores[5].start()
    for load, store in zip(loads, stores):
        load.wait()
        store.start()
    for store in stores:
        store.wait()


def per_device(wavefunctions, potential, occupation):
    in_hbm = pl.BlockSpec(memory_space=pltpu.HBM)
    vmem = pl.BlockSpec(memory_space=pltpu.VMEM)
    block = (PLANES, OWN_ROWS, GRID)
    planes = (2, 2, PLANES, GRID, GRID)
    dma = pltpu.SemaphoreType.DMA
    moved, summed = pl.pallas_call(
        kernel,
        name="taylor_step",
        out_shape=(
            jax.ShapeDtypeStruct(planes, F32),
            jax.ShapeDtypeStruct((2, *block), F32),
        ),
        in_specs=[in_hbm] * 5,
        out_specs=(in_hbm, vmem),
        scratch_shapes=[
            pltpu.SMEM((2,), F32),
            pltpu.VMEM(planes, F32),
            pltpu.VMEM((PLANES, GRID, GRID), F32),
            pltpu.VMEM((GRID, 3 * GRID), BF16),
            pltpu.VMEM((3 * GRID, GRID), BF16),
            pltpu.VMEM(planes, F32),
            pltpu.VMEM(planes, F32),
            pltpu.VMEM((4, GRID, ROWS, GRID), F32),
            pltpu.VMEM((GRID, ROWS, GRID), F32),
            pltpu.VMEM((2, GRID, ROWS, GRID), F32),
            pltpu.VMEM(planes, F32),
            pltpu.VMEM((PLANES, GRID, GRID), F32),
            pltpu.VMEM((BAND, *block), F32),
            pltpu.VMEM(block, F32),
            pltpu.VMEM((2, 2, OWN_ROWS, GRID), F32),
            pltpu.VMEM((2, PLANES, 2, GRID), F32),
            pltpu.VMEM((2, PLANES, 2, GRID), F32),
            pltpu.VMEM((PLANES, 32, GRID), F32),
            dma((5,)),
            dma((2,)),
            dma,
            dma((2,)),
            dma,
            dma((BAND,)),
            dma((2,)),
            dma,
            dma((4,)),
            dma((10,)),
        ],
        compiler_params=pltpu.CompilerParams(
            collective_id=0, has_side_effects=True, vmem_limit_bytes=67043328
        ),
    )(occupation, wavefunctions, potential, *kinetic_parts())
    return pl.pallas_call(
        finish,
        name="exchange",
        out_shape=(
            jax.ShapeDtypeStruct(planes, F32),
            jax.ShapeDtypeStruct(block, F32),
            jax.ShapeDtypeStruct(block, F32),
        ),
        in_specs=[in_hbm, in_hbm],
        out_specs=(in_hbm, in_hbm, in_hbm),
        scratch_shapes=[
            pltpu.VMEM((4, PLANES, GRID, GRID), F32),
            pltpu.VMEM((2, *block), F32),
            pltpu.VMEM((2, *block), F32),
            dma((5,)),
            dma((6,)),
        ],
        compiler_params=pltpu.CompilerParams(vmem_limit_bytes=67043328),
    )(moved, summed)


def solution(mesh):
    in_specs = (P(None, "band", "fft", None, None), P("fft", None, None), P("band"))
    out_specs = (P(None, "band", "fft", None, None), P("fft", "band", None), P("fft", "band", None))
    return jax.shard_map(
        per_device, mesh=mesh, in_specs=in_specs, out_specs=out_specs, check_vma=False
    )
```

```python
import functools
import math

import jax
import jax.numpy as jnp
import numpy as np
from jax import lax
from jax.experimental import pallas as pl
from jax.experimental.pallas import tpu as pltpu
from jax.sharding import PartitionSpec as P

SPACING = 0.4
TIME_STEP = 0.012
HALF_SQUARE = 0.5 * TIME_STEP * TIME_STEP
KAPPA_PBE = 0.804
MU_PBE = 0.21951
FERMI_FACTOR = 2.0 * math.pow(3.0 * math.pi * math.pi, 1.0 / 3.0)
SLATER_FACTOR = 0.75 * math.pow(3.0 / math.pi, 1.0 / 3.0)

GRID = 128
FFT = 32
BAND = 8
PLANES = GRID // FFT
ROWS = 8
OWN_ROWS = GRID // BAND
MESH = pl.DeviceIdType.MESH
F32 = jnp.float32
BF16 = jnp.bfloat16


def kinetic_matrix():
    counter = np.arange(GRID)
    signed = np.where(counter < GRID // 2, counter, counter - GRID)
    half_squares = 0.5 * (2.0 * np.pi * signed / (GRID * SPACING)) ** 2
    phase = np.outer(counter, counter) % GRID
    column = np.cos(2.0 * np.pi * phase / GRID) @ half_squares / GRID
    return column[(counter[:, None] - counter[None, :]) % GRID]


def kinetic_parts():
    matrix = kinetic_matrix()
    high = matrix.astype(jnp.bfloat16)
    low = (matrix - high.astype(np.float64)).astype(jnp.bfloat16)
    beside = np.concatenate([high, high, low], axis=1)
    return beside, beside.T.copy()


def split(values):
    high = values.astype(BF16)
    return high, (values - high.astype(F32)).astype(BF16)


def dot(a, b):
    return jnp.dot(a, b, preferred_element_type=F32)


def from_left(left, values):
    high, low = split(values)
    return dot(left, jnp.concatenate([high, low, high], axis=0))


def in_plane(left, right, values):
    high, low = split(values)
    return dot(left, jnp.concatenate([high, low, high], axis=0)) + dot(
        jnp.concatenate([high, low, high], axis=1), right
    )


def wait_bytes(ref, sem):
    pltpu.make_async_copy(ref, ref, sem).wait()


def kernel(
    occ_hbm,
    psi_hbm,
    pot_hbm,
    left_hbm,
    right_hbm,
    local,
    summed_ref,
    occ,
    psi,
    pot,
    left_table,
    right_table,
    tang,
    col,
    col_pot,
    back,
    ret,
    part,
    arrived,
    dens,
    halo_z,
    edge_x,
    halo_x,
    rows_x,
    sem_in,
    sem_col,
    sem_tang,
    sem_ret,
    sem_group,
    sem_pot,
    sem_dens,
    sem_halo,
    send,
):
    me = lax.axis_index("fft")
    my_band = lax.axis_index("band")
    my_slot = me // 2
    my_chip = me // 4

    def fft_peer(step):
        k = (step + 1) // 2
        sign = 2 * (step % 2) - 1
        return lax.rem(me + sign * k + FFT, FFT)

    def rows_of(slot):
        return pl.ds(pl.multiple_of(slot * ROWS, ROWS), ROWS)

    def planes_of(device):
        return pl.ds(device * PLANES, PLANES)

    loads = [
        pltpu.make_async_copy(source, target, sem_in.at[k])
        for k, (source, target) in enumerate((
            (psi_hbm, psi),
            (pot_hbm, pot),
            (left_hbm, left_table),
            (right_hbm, right_table),
            (occ_hbm, occ),
        ))
    ]
    for load in loads:
        load.start()
    barrier = pltpu.get_barrier_semaphore()

    def sign_of(step):
        half = step // 2
        return FFT + (2 * (step % 2) - 1) * half

    @pl.loop(1, FFT)
    def _(step):
        pl.semaphore_signal(
            barrier,
            inc=1,
            device_id={"fft": lax.rem(me + FFT // 2 + sign_of(step), FFT)},
            device_id_type=MESH,
        )

    @pl.loop(1, BAND)
    def _(step):
        pl.semaphore_signal(
            barrier,
            inc=1,
            device_id={"band": lax.rem(my_band + step, BAND)},
            device_id_type=MESH,
        )

    @pl.loop(1, BAND)
    def _(step):
        pl.semaphore_signal(
            barrier,
            inc=1,
            device_id={
                "fft": me + 1 - 2 * (me % 2),
                "band": lax.rem(my_band + step, BAND),
            },
            device_id_type=MESH,
        )

    for load in loads:
        load.wait()
    pl.semaphore_wait(barrier, FFT - 1 + 2 * (BAND - 1))

    first_slot = lax.rem(my_band - me + FFT, BAND)
    for k in range(2):
        target = 2 * (first_slot + BAND * k) + (me // BAND) % 2

        @pl.when(target != me)
        def _():
            pltpu.make_async_remote_copy(
                src_ref=pot.at[:, rows_of(target // 2), :],
                dst_ref=col_pot.at[planes_of(me)],
                send_sem=send.at[1],
                recv_sem=sem_pot.at[0],
                device_id={"fft": target},
                device_id_type=MESH,
            ).start()

        @pl.when(target == me)
        def _():
            pltpu.make_async_copy(
                pot.at[:, rows_of(my_slot), :],
                col_pot.at[planes_of(me)],
                sem_pot.at[0],
            ).start()

    @pl.loop(1, FFT)
    def _(step):
        peer = fft_peer(step)
        pltpu.make_async_remote_copy(
            src_ref=psi.at[:, peer % 2, :, rows_of(peer // 2), :],
            dst_ref=col.at[pl.ds(0, 2), planes_of(me)],
            send_sem=send.at[0],
            recv_sem=sem_col,
            device_id={"fft": peer},
            device_id_type=MESH,
        ).start()

    pltpu.make_async_copy(
        psi.at[:, me % 2, :, rows_of(my_slot), :],
        col.at[pl.ds(0, 2), planes_of(me)],
        sem_col,
    ).start()

    left, right = left_table[...], right_table[...]

    for part_of in range(2):

        @pl.loop(0, 8, unroll=4)
        def _(index):
            band, plane = index // 4, index % 4
            tang[part_of, band, plane] = in_plane(left, right, psi[part_of, band, plane])

        @pl.loop(1, FFT)
        def _(step):
            peer = fft_peer(step)
            pltpu.make_async_remote_copy(
                src_ref=tang.at[part_of, peer % 2, :, rows_of(peer // 2), :],
                dst_ref=col.at[2 + part_of, planes_of(me)],
                send_sem=send.at[2],
                recv_sem=sem_tang.at[part_of],
                device_id={"fft": peer},
                device_id_type=MESH,
            ).start()

        pltpu.make_async_copy(
            tang.at[part_of, me % 2, :, rows_of(my_slot), :],
            col.at[2 + part_of, planes_of(me)],
            sem_tang.at[part_of],
        ).start()

    wait_bytes(col_pot.at[pl.ds(0, 8)], sem_pot.at[0])
    first_device = lax.rem(my_band - my_slot + FFT, BAND) + BAND * (me % 2)

    @pl.loop(0, 2)
    def _(k):
        held = planes_of(first_device + 2 * BAND * k)

        @pl.loop(1, 2 * BAND)
        def _(step):
            seat = lax.rem(2 * my_band + me % 2 + step, 2 * BAND)
            pltpu.make_async_remote_copy(
                src_ref=col_pot.at[held],
                dst_ref=col_pot.at[held],
                send_sem=send.at[3],
                recv_sem=sem_pot.at[1],
                device_id={"fft": 2 * my_slot + seat % 2, "band": seat // 2},
                device_id_type=MESH,
            ).start()

    @pl.loop(0, 8, unroll=2)
    def _(index):
        band, plane = index // 4, index % 4
        values = pot[plane]
        real, imag = psi[0, band, plane], psi[1, band, plane]
        first_real = tang[0, band, plane] + values * real
        first_imag = tang[1, band, plane] + values * imag
        second_real = in_plane(left, right, first_real) + values * first_real
        second_imag = in_plane(left, right, first_imag) + values * first_imag
        local[0, band, plane] = real + TIME_STEP * first_imag - HALF_SQUARE * second_real
        local[1, band, plane] = imag - TIME_STEP * first_real - HALF_SQUARE * second_imag

    wait_bytes(col.at[pl.ds(0, 2)], sem_col)
    wait_bytes(col_pot.at[pl.ds(0, 120)], sem_pot.at[1])
    for part_of in range(2):
        sign = 1.0 - 2.0 * part_of
        wait_bytes(col.at[2 + part_of], sem_tang.at[part_of])

        for pair in range(0, ROWS, 2):

            def rows(ref, *index):
                return jnp.concatenate(
                    [ref[(*index, slice(None), pair + k)] for k in range(2)], axis=1
                )

            values = rows(col_pot)
            mine = rows(col, part_of)
            along = from_left(left, mine)
            inner = (
                (sign * TIME_STEP) * rows(col, 1 - part_of)
                - (2.0 * HALF_SQUARE) * rows(col, 2 + part_of)
                - HALF_SQUARE * (values * mine + along)
            )
            moved = from_left(left, inner) - HALF_SQUARE * (values * along)
            for k in range(2):
                back[part_of, :, pair + k, :] = moved[:, k * GRID : (k + 1) * GRID]

        @pl.loop(1, FFT)
        def _(step):
            peer = fft_peer(step)
            pltpu.make_async_remote_copy(
                src_ref=back.at[part_of, planes_of(peer)],
                dst_ref=ret.at[part_of, me % 2, :, rows_of(my_slot), :],
                send_sem=send.at[4],
                recv_sem=sem_ret if part_of == 0 else sem_group.at[my_chip],
                device_id={"fft": peer},
                device_id_type=MESH,
            ).start()

        pltpu.make_async_copy(
            back.at[part_of, planes_of(me)],
            ret.at[part_of, me % 2, :, rows_of(my_slot), :],
            sem_ret if part_of == 0 else sem_group.at[my_chip],
        ).start()

    wait_bytes(ret.at[0], sem_ret)

    @pl.loop(0, PLANES)
    def _(plane):
        low = local[0, 0, plane] + ret[0, 0, plane]
        high = local[0, 1, plane] + ret[0, 1, plane]
        local[0, 0, plane] = low
        local[0, 1, plane] = high
        part[plane] = occ[0] * (low * low) + occ[1] * (high * high)

    @pl.loop(0, BAND)
    def _(step):
        k = (step + 1) // 2
        sign = 2 * (step % 2) - 1
        block = lax.rem(my_chip + sign * k + BAND, BAND)
        rows = pl.ds(pl.multiple_of(block * OWN_ROWS, OWN_ROWS), OWN_ROWS)
        wait_bytes(ret.at[1, :, :, pl.ds(0, OWN_ROWS), :], sem_group.at[block])
        low = local[1, 0, :, rows, :] + ret[1, 0, :, rows, :]
        high = local[1, 1, :, rows, :] + ret[1, 1, :, rows, :]
        local[1, 0, :, rows, :] = low
        local[1, 1, :, rows, :] = high
        part[:, rows, :] = part[:, rows, :] + (occ[0] * (low * low) + occ[1] * (high * high))

        @pl.when(block != my_band)
        def _():
            pltpu.make_async_remote_copy(
                src_ref=part.at[:, rows, :],
                dst_ref=arrived.at[my_band],
                send_sem=send.at[5],
                recv_sem=sem_dens,
                device_id={"band": block},
                device_id_type=MESH,
            ).start()

        @pl.when(block == my_band)
        def _():
            pltpu.make_async_copy(part.at[:, rows, :], arrived.at[my_band], sem_dens).start()

    wait_bytes(arrived, sem_dens)
    total = arrived[0]
    for k in range(1, BAND):
        total = total + arrived[k]
    dens[...] = total
    rows_x[:, 8:24, :] = total
    edge_x[0] = dens[:, 14:16, :]
    edge_x[1] = dens[:, 0:2, :]

    halos = []
    for side in range(2):
        shift = 1 - 2 * side
        halos.append(
            pltpu.make_async_remote_copy(
                src_ref=dens.at[pl.ds(2 - 2 * side, 2)],
                dst_ref=halo_z.at[side],
                send_sem=send.at[6 + side],
                recv_sem=sem_halo.at[side],
                device_id={"fft": lax.rem(me + shift + FFT, FFT)},
                device_id_type=MESH,
            )
        )
        halos.append(
            pltpu.make_async_remote_copy(
                src_ref=edge_x.at[side],
                dst_ref=halo_x.at[side],
                send_sem=send.at[8 + side],
                recv_sem=sem_halo.at[2 + side],
                device_id={"band": lax.rem(my_band + shift + BAND, BAND)},
                device_id_type=MESH,
            )
        )
    for halo in halos:
        halo.start()

    scale = 1.0 / (12.0 * SPACING)
    grad_y = (
        8.0 * (pltpu.roll(total, GRID - 1, 2) - pltpu.roll(total, 1, 2))
        - (pltpu.roll(total, GRID - 2, 2) - pltpu.roll(total, 2, 2))
    ) * scale

    wait_bytes(col.at[pl.ds(0, 2), pl.ds(0, 124)], send.at[0])
    wait_bytes(col.at[pl.ds(0, 2), pl.ds(0, 124)], send.at[2])
    wait_bytes(back.at[:, pl.ds(0, 124)], send.at[4])
    wait_bytes(col_pot.at[pl.ds(0, 120)], send.at[3])
    wait_bytes(arrived.at[pl.ds(0, 7)], send.at[5])
    holds_own = jnp.logical_and(
        lax.rem(me + my_slot - my_band + FFT, BAND) == 0, me % 2 == (me // BAND) % 2
    )

    @pl.when(holds_own)
    def _():
        wait_bytes(col_pot.at[pl.ds(0, 4)], send.at[1])

    @pl.when(jnp.logical_not(holds_own))
    def _():
        wait_bytes(col_pot.at[pl.ds(0, 8)], send.at[1])

    for halo in halos:
        halo.wait()
    rows_x[:, 6:8, :] = halo_x[0]
    rows_x[:, 24:26, :] = halo_x[1]
    grad_x = (
        8.0 * (rows_x[:, 9:25, :] - rows_x[:, 7:23, :])
        - (rows_x[:, 10:26, :] - rows_x[:, 6:22, :])
    ) * scale
    stack = jnp.concatenate([halo_z[0], total, halo_z[1]], axis=0)
    grad_z = (8.0 * (stack[3:7] - stack[1:5]) - (stack[4:8] - stack[0:4])) * scale
    summed_ref[0] = grad_z * grad_z + grad_x * grad_x + grad_y * grad_y
    summed_ref[1] = total


def exchange_terms(square, density):
    power = jnp.exp((4.0 / 3.0) * jnp.log(density))
    reduced = jnp.sqrt(square) / (FERMI_FACTOR * power)
    enhance = 1.0 + KAPPA_PBE - KAPPA_PBE / (1.0 + MU_PBE * reduced * reduced / KAPPA_PBE)
    return reduced, -SLATER_FACTOR * power * enhance


def finish(moved, summed, moved_out, reduced_out, energy_out, terms, sem_out):
    stores = [
        pltpu.make_async_copy(moved.at[k // 2, k % 2], moved_out.at[k // 2, k % 2], sem_out.at[k])
        for k in range(4)
    ]
    stores.append(pltpu.make_async_copy(terms.at[0], reduced_out, sem_out.at[4]))
    stores.append(pltpu.make_async_copy(terms.at[1], energy_out, sem_out.at[5]))
    for store in stores[:4]:
        store.start()
    terms[0], terms[1] = exchange_terms(summed[0], summed[1])
    for store in stores[4:]:
        store.start()
    for store in stores:
        store.wait()


def per_device(wavefunctions, potential, occupation):
    in_hbm = pl.BlockSpec(memory_space=pltpu.HBM)
    vmem = pl.BlockSpec(memory_space=pltpu.VMEM)
    block = (PLANES, OWN_ROWS, GRID)
    planes = (2, 2, PLANES, GRID, GRID)
    dma = pltpu.SemaphoreType.DMA
    moved, summed = pl.pallas_call(
        kernel,
        name="taylor_step",
        out_shape=(
            pltpu.VMEM(planes, F32),
            pltpu.VMEM((2, *block), F32),
        ),
        in_specs=[in_hbm] * 5,
        out_specs=(vmem, vmem),
        scratch_shapes=[
            pltpu.SMEM((2,), F32),
            pltpu.VMEM(planes, F32),
            pltpu.VMEM((PLANES, GRID, GRID), F32),
            pltpu.VMEM((GRID, 3 * GRID), BF16),
            pltpu.VMEM((3 * GRID, GRID), BF16),
            pltpu.VMEM(planes, F32),
            pltpu.VMEM((4, GRID, ROWS, GRID), F32),
            pltpu.VMEM((GRID, ROWS, GRID), F32),
            pltpu.VMEM((2, GRID, ROWS, GRID), F32),
            pltpu.VMEM(planes, F32),
            pltpu.VMEM((PLANES, GRID, GRID), F32),
            pltpu.VMEM((BAND, *block), F32),
            pltpu.VMEM(block, F32),
            pltpu.VMEM((2, 2, OWN_ROWS, GRID), F32),
            pltpu.VMEM((2, PLANES, 2, GRID), F32),
            pltpu.VMEM((2, PLANES, 2, GRID), F32),
            pltpu.VMEM((PLANES, 32, GRID), F32),
            dma((5,)),
            dma,
            dma((2,)),
            dma,
            dma((BAND,)),
            dma((2,)),
            dma,
            dma((4,)),
            dma((10,)),
        ],
        compiler_params=pltpu.CompilerParams(
            collective_id=0, has_side_effects=True, vmem_limit_bytes=62000000
        ),
    )(occupation, wavefunctions, potential, *kinetic_parts())
    return pl.pallas_call(
        finish,
        name="exchange",
        out_shape=(
            jax.ShapeDtypeStruct(planes, F32),
            jax.ShapeDtypeStruct(block, F32),
            jax.ShapeDtypeStruct(block, F32),
        ),
        in_specs=[vmem, vmem],
        out_specs=(in_hbm, in_hbm, in_hbm),
        scratch_shapes=[
            pltpu.VMEM((2, *block), F32),
            dma((6,)),
        ],
        compiler_params=pltpu.CompilerParams(vmem_limit_bytes=16000000),
    )(moved, summed)


def solution(mesh):
    in_specs = (P(None, "band", "fft", None, None), P("fft", None, None), P("band"))
    out_specs = (P(None, "band", "fft", None, None), P("fft", "band", None), P("fft", "band", None))
    return jax.shard_map(
        per_device, mesh=mesh, in_specs=in_specs, out_specs=out_specs, check_vma=False
    )
```

```python
import functools
import math

import jax
import jax.numpy as jnp
import numpy as np
from jax import lax
from jax.experimental import pallas as pl
from jax.experimental.pallas import tpu as pltpu
from jax.sharding import PartitionSpec as P

SPACING = 0.4
TIME_STEP = 0.012
HALF_SQUARE = 0.5 * TIME_STEP * TIME_STEP
KAPPA_PBE = 0.804
MU_PBE = 0.21951
FERMI_FACTOR = 2.0 * math.pow(3.0 * math.pi * math.pi, 1.0 / 3.0)
SLATER_FACTOR = 0.75 * math.pow(3.0 / math.pi, 1.0 / 3.0)

GRID = 128
FFT = 32
BAND = 8
PLANES = GRID // FFT
ROWS = 8
OWN_ROWS = GRID // BAND
MESH = pl.DeviceIdType.MESH
F32 = jnp.float32
BF16 = jnp.bfloat16


def kinetic_matrix():
    counter = np.arange(GRID)
    signed = np.where(counter < GRID // 2, counter, counter - GRID)
    half_squares = 0.5 * (2.0 * np.pi * signed / (GRID * SPACING)) ** 2
    phase = np.outer(counter, counter) % GRID
    column = np.cos(2.0 * np.pi * phase / GRID) @ half_squares / GRID
    return column[(counter[:, None] - counter[None, :]) % GRID]


def kinetic_parts():
    matrix = kinetic_matrix()
    high = matrix.astype(jnp.bfloat16)
    low = (matrix - high.astype(np.float64)).astype(jnp.bfloat16)
    beside = np.concatenate([high, high, low], axis=1)
    return beside, beside.T.copy()


def split(values):
    high = values.astype(BF16)
    return high, (values - high.astype(F32)).astype(BF16)


def dot(a, b):
    return jnp.dot(a, b, preferred_element_type=F32)


def from_left(left, values):
    high, low = split(values)
    return dot(left, jnp.concatenate([high, low, high], axis=0))


def in_plane(left, right, values):
    high, low = split(values)
    return dot(left, jnp.concatenate([high, low, high], axis=0)) + dot(
        jnp.concatenate([high, low, high], axis=1), right
    )


def wait_bytes(ref, sem):
    pltpu.make_async_copy(ref, ref, sem).wait()


def kernel(
    occ_hbm,
    psi_hbm,
    pot_hbm,
    left_hbm,
    right_hbm,
    local,
    summed_ref,
    occ,
    psi,
    pot,
    left_table,
    right_table,
    tang,
    col,
    col_pot,
    back,
    ret,
    part,
    arrived,
    dens,
    halo_z,
    edge_x,
    halo_x,
    rows_x,
    sem_in,
    sem_col,
    sem_tang,
    sem_ret,
    sem_group,
    sem_pot,
    sem_dens,
    sem_halo,
    send,
    sem_group_in,
    sem_groups_in,
):
    me = lax.axis_index("fft")
    my_band = lax.axis_index("band")
    my_slot = me // 2
    my_chip = me // 4

    def fft_peer(step):
        k = (step + 1) // 2
        sign = 2 * (step % 2) - 1
        return lax.rem(me + sign * k + FFT, FFT)

    def rows_of(slot):
        return pl.ds(pl.multiple_of(slot * ROWS, ROWS), ROWS)

    def planes_of(device):
        return pl.ds(device * PLANES, PLANES)

    loads = [
        pltpu.make_async_copy(source, target, sem_in.at[k])
        for k, (source, target) in enumerate((
            (psi_hbm, psi),
            (pot_hbm, pot),
            (left_hbm, left_table),
            (right_hbm, right_table),
            (occ_hbm, occ),
        ))
    ]
    for load in loads:
        load.start()
    barrier = pltpu.get_barrier_semaphore()

    def sign_of(step):
        half = step // 2
        return FFT + (2 * (step % 2) - 1) * half

    @pl.loop(1, FFT)
    def _(step):
        pl.semaphore_signal(
            barrier,
            inc=1,
            device_id={"fft": lax.rem(me + FFT // 2 + sign_of(step), FFT)},
            device_id_type=MESH,
        )

    stands = jnp.logical_and(me >= 1, me < BAND)
    ahead = {"band": lax.rem(my_band + me, BAND)}
    behind = {"band": lax.rem(my_band - me + FFT, BAND)}

    @pl.when(stands)
    def _():
        pl.semaphore_signal(barrier, inc=1, device_id=ahead, device_id_type=MESH)

    for load in loads:
        load.wait()
    @pl.when(jnp.logical_not(stands))
    def _():
        pl.semaphore_wait(barrier, FFT - 1)

    @pl.when(stands)
    def _():
        pl.semaphore_wait(barrier, FFT)
        pl.semaphore_signal(sem_group_in, inc=1, device_id=behind, device_id_type=MESH)


    first_slot = lax.rem(my_band - me + FFT, BAND)
    for k in range(2):
        target = 2 * (first_slot + BAND * k) + (me // BAND) % 2

        @pl.when(target != me)
        def _():
            pltpu.make_async_remote_copy(
                src_ref=pot.at[:, rows_of(target // 2), :],
                dst_ref=col_pot.at[planes_of(me)],
                send_sem=send.at[1],
                recv_sem=sem_pot.at[0],
                device_id={"fft": target},
                device_id_type=MESH,
            ).start()

        @pl.when(target == me)
        def _():
            pltpu.make_async_copy(
                pot.at[:, rows_of(my_slot), :],
                col_pot.at[planes_of(me)],
                sem_pot.at[0],
            ).start()

    @pl.loop(1, FFT)
    def _(step):
        peer = fft_peer(step)
        pltpu.make_async_remote_copy(
            src_ref=psi.at[:, peer % 2, :, rows_of(peer // 2), :],
            dst_ref=col.at[pl.ds(0, 2), planes_of(me)],
            send_sem=send.at[0],
            recv_sem=sem_col,
            device_id={"fft": peer},
            device_id_type=MESH,
        ).start()

    pltpu.make_async_copy(
        psi.at[:, me % 2, :, rows_of(my_slot), :],
        col.at[pl.ds(0, 2), planes_of(me)],
        sem_col,
    ).start()

    left, right = left_table[...], right_table[...]

    for part_of in range(2):

        @pl.loop(0, 8, unroll=4)
        def _(index):
            band, plane = index // 4, index % 4
            tang[part_of, band, plane] = in_plane(left, right, psi[part_of, band, plane])

        @pl.loop(1, FFT)
        def _(step):
            peer = fft_peer(step)
            pltpu.make_async_remote_copy(
                src_ref=tang.at[part_of, peer % 2, :, rows_of(peer // 2), :],
                dst_ref=col.at[2 + part_of, planes_of(me)],
                send_sem=send.at[2],
                recv_sem=sem_tang.at[part_of],
                device_id={"fft": peer},
                device_id_type=MESH,
            ).start()

        pltpu.make_async_copy(
            tang.at[part_of, me % 2, :, rows_of(my_slot), :],
            col.at[2 + part_of, planes_of(me)],
            sem_tang.at[part_of],
        ).start()

    @pl.when(stands)
    def _():
        pl.semaphore_wait(sem_group_in, 1)
        pl.semaphore_signal(sem_groups_in, inc=1)

        @pl.loop(1, FFT)
        def _(step):
            pl.semaphore_signal(
                sem_groups_in,
                inc=1,
                device_id={"fft": lax.rem(me + step, FFT)},
                device_id_type=MESH,
            )

    pl.semaphore_wait(sem_groups_in, BAND - 1)

    wait_bytes(col_pot.at[pl.ds(0, 8)], sem_pot.at[0])
    first_device = lax.rem(my_band - my_slot + FFT, BAND) + BAND * (me % 2)

    @pl.loop(0, 2)
    def _(k):
        held = planes_of(first_device + 2 * BAND * k)

        @pl.loop(1, 2 * BAND)
        def _(step):
            seat = lax.rem(2 * my_band + me % 2 + step, 2 * BAND)
            pltpu.make_async_remote_copy(
                src_ref=col_pot.at[held],
                dst_ref=col_pot.at[held],
                send_sem=send.at[3],
                recv_sem=sem_pot.at[1],
                device_id={"fft": 2 * my_slot + seat % 2, "band": seat // 2},
                device_id_type=MESH,
            ).start()

    @pl.loop(0, 8, unroll=2)
    def _(index):
        band, plane = index // 4, index % 4
        values = pot[plane]
        real, imag = psi[0, band, plane], psi[1, band, plane]
        first_real = tang[0, band, plane] + values * real
        first_imag = tang[1, band, plane] + values * imag
        second_real = in_plane(left, right, first_real) + values * first_real
        second_imag = in_plane(left, right, first_imag) + values * first_imag
        local[0, band, plane] = real + TIME_STEP * first_imag - HALF_SQUARE * second_real
        local[1, band, plane] = imag - TIME_STEP * first_real - HALF_SQUARE * second_imag

    wait_bytes(col.at[pl.ds(0, 2)], sem_col)
    wait_bytes(col_pot.at[pl.ds(0, 120)], sem_pot.at[1])
    for part_of in range(2):
        sign = 1.0 - 2.0 * part_of
        wait_bytes(col.at[2 + part_of], sem_tang.at[part_of])

        for pair in range(0, ROWS, 2):

            def rows(ref, *index):
                return jnp.concatenate(
                    [ref[(*index, slice(None), pair + k)] for k in range(2)], axis=1
                )

            values = rows(col_pot)
            mine = rows(col, part_of)
            along = from_left(left, mine)
            inner = (
                (sign * TIME_STEP) * rows(col, 1 - part_of)
                - (2.0 * HALF_SQUARE) * rows(col, 2 + part_of)
                - HALF_SQUARE * (values * mine + along)
            )
            moved = from_left(left, inner) - HALF_SQUARE * (values * along)
            for k in range(2):
                back[part_of, :, pair + k, :] = moved[:, k * GRID : (k + 1) * GRID]

        @pl.loop(1, FFT)
        def _(step):
            peer = fft_peer(step)
            pltpu.make_async_remote_copy(
                src_ref=back.at[part_of, planes_of(peer)],
                dst_ref=ret.at[part_of, me % 2, :, rows_of(my_slot), :],
                send_sem=send.at[4],
                recv_sem=sem_ret if part_of == 0 else sem_group.at[my_chip],
                device_id={"fft": peer},
                device_id_type=MESH,
            ).start()

        pltpu.make_async_copy(
            back.at[part_of, planes_of(me)],
            ret.at[part_of, me % 2, :, rows_of(my_slot), :],
            sem_ret if part_of == 0 else sem_group.at[my_chip],
        ).start()

    wait_bytes(ret.at[0], sem_ret)

    @pl.loop(0, PLANES)
    def _(plane):
        low = local[0, 0, plane] + ret[0, 0, plane]
        high = local[0, 1, plane] + ret[0, 1, plane]
        local[0, 0, plane] = low
        local[0, 1, plane] = high
        part[plane] = occ[0] * (low * low) + occ[1] * (high * high)

    @pl.loop(0, BAND)
    def _(step):
        k = (step + 1) // 2
        sign = 2 * (step % 2) - 1
        block = lax.rem(my_chip + sign * k + BAND, BAND)
        rows = pl.ds(pl.multiple_of(block * OWN_ROWS, OWN_ROWS), OWN_ROWS)
        wait_bytes(ret.at[1, :, :, pl.ds(0, OWN_ROWS), :], sem_group.at[block])
        low = local[1, 0, :, rows, :] + ret[1, 0, :, rows, :]
        high = local[1, 1, :, rows, :] + ret[1, 1, :, rows, :]
        local[1, 0, :, rows, :] = low
        local[1, 1, :, rows, :] = high
        part[:, rows, :] = part[:, rows, :] + (occ[0] * (low * low) + occ[1] * (high * high))

        @pl.when(block != my_band)
        def _():
            pltpu.make_async_remote_copy(
                src_ref=part.at[:, rows, :],
                dst_ref=arrived.at[my_band],
                send_sem=send.at[5],
                recv_sem=sem_dens,
                device_id={"band": block},
                device_id_type=MESH,
            ).start()

        @pl.when(block == my_band)
        def _():
            pltpu.make_async_copy(part.at[:, rows, :], arrived.at[my_band], sem_dens).start()

    wait_bytes(arrived, sem_dens)
    total = arrived[0]
    for k in range(1, BAND):
        total = total + arrived[k]
    dens[...] = total
    rows_x[:, 8:24, :] = total
    edge_x[0] = dens[:, 14:16, :]
    edge_x[1] = dens[:, 0:2, :]

    halos = []
    for side in range(2):
        shift = 1 - 2 * side
        halos.append(
            pltpu.make_async_remote_copy(
                src_ref=dens.at[pl.ds(2 - 2 * side, 2)],
                dst_ref=halo_z.at[side],
                send_sem=send.at[6 + side],
                recv_sem=sem_halo.at[side],
                device_id={"fft": lax.rem(me + shift + FFT, FFT)},
                device_id_type=MESH,
            )
        )
        halos.append(
            pltpu.make_async_remote_copy(
                src_ref=edge_x.at[side],
                dst_ref=halo_x.at[side],
                send_sem=send.at[8 + side],
                recv_sem=sem_halo.at[2 + side],
                device_id={"band": lax.rem(my_band + shift + BAND, BAND)},
                device_id_type=MESH,
            )
        )
    for halo in halos:
        halo.start()

    scale = 1.0 / (12.0 * SPACING)
    grad_y = (
        8.0 * (pltpu.roll(total, GRID - 1, 2) - pltpu.roll(total, 1, 2))
        - (pltpu.roll(total, GRID - 2, 2) - pltpu.roll(total, 2, 2))
    ) * scale

    wait_bytes(col.at[pl.ds(0, 2), pl.ds(0, 124)], send.at[0])
    wait_bytes(col.at[pl.ds(0, 2), pl.ds(0, 124)], send.at[2])
    wait_bytes(back.at[:, pl.ds(0, 124)], send.at[4])
    wait_bytes(col_pot.at[pl.ds(0, 120)], send.at[3])
    wait_bytes(arrived.at[pl.ds(0, 7)], send.at[5])
    holds_own = jnp.logical_and(
        lax.rem(me + my_slot - my_band + FFT, BAND) == 0, me % 2 == (me // BAND) % 2
    )

    @pl.when(holds_own)
    def _():
        wait_bytes(col_pot.at[pl.ds(0, 4)], send.at[1])

    @pl.when(jnp.logical_not(holds_own))
    def _():
        wait_bytes(col_pot.at[pl.ds(0, 8)], send.at[1])

    for halo in halos:
        halo.wait()
    rows_x[:, 6:8, :] = halo_x[0]
    rows_x[:, 24:26, :] = halo_x[1]
    grad_x = (
        8.0 * (rows_x[:, 9:25, :] - rows_x[:, 7:23, :])
        - (rows_x[:, 10:26, :] - rows_x[:, 6:22, :])
    ) * scale
    stack = jnp.concatenate([halo_z[0], total, halo_z[1]], axis=0)
    grad_z = (8.0 * (stack[3:7] - stack[1:5]) - (stack[4:8] - stack[0:4])) * scale
    summed_ref[0] = grad_z * grad_z + grad_x * grad_x + grad_y * grad_y
    summed_ref[1] = total


def exchange_terms(square, density):
    power = jnp.exp((4.0 / 3.0) * jnp.log(density))
    reduced = jnp.sqrt(square) / (FERMI_FACTOR * power)
    enhance = 1.0 + KAPPA_PBE - KAPPA_PBE / (1.0 + MU_PBE * reduced * reduced / KAPPA_PBE)
    return reduced, -SLATER_FACTOR * power * enhance


def finish(moved, summed, moved_out, reduced_out, energy_out, terms, sem_out):
    stores = [
        pltpu.make_async_copy(moved.at[k // 2, k % 2], moved_out.at[k // 2, k % 2], sem_out.at[k])
        for k in range(4)
    ]
    stores.append(pltpu.make_async_copy(terms.at[0], reduced_out, sem_out.at[4]))
    stores.append(pltpu.make_async_copy(terms.at[1], energy_out, sem_out.at[5]))
    for store in stores[:4]:
        store.start()
    terms[0], terms[1] = exchange_terms(summed[0], summed[1])
    for store in stores[4:]:
        store.start()
    for store in stores:
        store.wait()


def per_device(wavefunctions, potential, occupation):
    in_hbm = pl.BlockSpec(memory_space=pltpu.HBM)
    vmem = pl.BlockSpec(memory_space=pltpu.VMEM)
    block = (PLANES, OWN_ROWS, GRID)
    planes = (2, 2, PLANES, GRID, GRID)
    dma = pltpu.SemaphoreType.DMA
    moved, summed = pl.pallas_call(
        kernel,
        name="taylor_step",
        out_shape=(
            pltpu.VMEM(planes, F32),
            pltpu.VMEM((2, *block), F32),
        ),
        in_specs=[in_hbm] * 5,
        out_specs=(vmem, vmem),
        scratch_shapes=[
            pltpu.SMEM((2,), F32),
            pltpu.VMEM(planes, F32),
            pltpu.VMEM((PLANES, GRID, GRID), F32),
            pltpu.VMEM((GRID, 3 * GRID), BF16),
            pltpu.VMEM((3 * GRID, GRID), BF16),
            pltpu.VMEM(planes, F32),
            pltpu.VMEM((4, GRID, ROWS, GRID), F32),
            pltpu.VMEM((GRID, ROWS, GRID), F32),
            pltpu.VMEM((2, GRID, ROWS, GRID), F32),
            pltpu.VMEM(planes, F32),
            pltpu.VMEM((PLANES, GRID, GRID), F32),
            pltpu.VMEM((BAND, *block), F32),
            pltpu.VMEM(block, F32),
            pltpu.VMEM((2, 2, OWN_ROWS, GRID), F32),
            pltpu.VMEM((2, PLANES, 2, GRID), F32),
            pltpu.VMEM((2, PLANES, 2, GRID), F32),
            pltpu.VMEM((PLANES, 32, GRID), F32),
            dma((5,)),
            dma,
            dma((2,)),
            dma,
            dma((BAND,)),
            dma((2,)),
            dma,
            dma((4,)),
            dma((10,)),
            pltpu.SemaphoreType.REGULAR,
            pltpu.SemaphoreType.REGULAR,
        ],
        compiler_params=pltpu.CompilerParams(
            collective_id=0, has_side_effects=True, vmem_limit_bytes=62000000
        ),
    )(occupation, wavefunctions, potential, *kinetic_parts())
    return pl.pallas_call(
        finish,
        name="exchange",
        out_shape=(
            jax.ShapeDtypeStruct(planes, F32),
            jax.ShapeDtypeStruct(block, F32),
            jax.ShapeDtypeStruct(block, F32),
        ),
        in_specs=[vmem, vmem],
        out_specs=(in_hbm, in_hbm, in_hbm),
        scratch_shapes=[
            pltpu.VMEM((2, *block), F32),
            dma((6,)),
        ],
        compiler_params=pltpu.CompilerParams(vmem_limit_bytes=16000000),
    )(moved, summed)


def solution(mesh):
    in_specs = (P(None, "band", "fft", None, None), P("fft", None, None), P("band"))
    out_specs = (P(None, "band", "fft", None, None), P("fft", "band", None), P("fft", "band", None))
    return jax.shard_map(
        per_device, mesh=mesh, in_specs=in_specs, out_specs=out_specs, check_vma=False
    )
```

```python
import functools
import math

import jax
import jax.numpy as jnp
import numpy as np
from jax import lax
from jax.experimental import pallas as pl
from jax.experimental.pallas import tpu as pltpu
from jax.sharding import PartitionSpec as P

SPACING = 0.4
TIME_STEP = 0.012
HALF_SQUARE = 0.5 * TIME_STEP * TIME_STEP
KAPPA_PBE = 0.804
MU_PBE = 0.21951
FERMI_FACTOR = 2.0 * math.pow(3.0 * math.pi * math.pi, 1.0 / 3.0)
SLATER_FACTOR = 0.75 * math.pow(3.0 / math.pi, 1.0 / 3.0)

GRID = 128
FFT = 32
BAND = 8
PLANES = GRID // FFT
ROWS = 8
OWN_ROWS = GRID // BAND
MESH = pl.DeviceIdType.MESH
F32 = jnp.float32
BF16 = jnp.bfloat16


def kinetic_matrix():
    counter = np.arange(GRID)
    signed = np.where(counter < GRID // 2, counter, counter - GRID)
    half_squares = 0.5 * (2.0 * np.pi * signed / (GRID * SPACING)) ** 2
    phase = np.outer(counter, counter) % GRID
    column = np.cos(2.0 * np.pi * phase / GRID) @ half_squares / GRID
    return column[(counter[:, None] - counter[None, :]) % GRID]


def kinetic_parts():
    matrix = kinetic_matrix()
    high = matrix.astype(jnp.bfloat16)
    low = (matrix - high.astype(np.float64)).astype(jnp.bfloat16)
    beside = np.concatenate([high, high, low], axis=1)
    return beside, beside.T.copy()


def split(values):
    high = values.astype(BF16)
    return high, (values - high.astype(F32)).astype(BF16)


def dot(a, b):
    return jnp.dot(a, b, preferred_element_type=F32)


def from_left(left, values):
    high, low = split(values)
    return dot(left, jnp.concatenate([high, low, high], axis=0))


def in_plane(left, right, values):
    high, low = split(values)
    return dot(left, jnp.concatenate([high, low, high], axis=0)) + dot(
        jnp.concatenate([high, low, high], axis=1), right
    )


def wait_bytes(ref, sem):
    pltpu.make_async_copy(ref, ref, sem).wait()


def kernel(
    occ_hbm,
    psi_hbm,
    pot_hbm,
    left_hbm,
    right_hbm,
    local,
    summed_ref,
    occ,
    psi,
    pot,
    left_table,
    right_table,
    tang,
    col,
    col_pot,
    back,
    ret,
    part,
    arrived,
    dens,
    halo_z,
    edge_x,
    halo_x,
    rows_x,
    sem_in,
    sem_col,
    sem_tang,
    sem_ret,
    sem_group,
    sem_pot,
    sem_dens,
    sem_halo,
    send,
    sem_group_in,
    sem_groups_in,
):
    me = lax.axis_index("fft")
    my_band = lax.axis_index("band")
    my_slot = me // 2
    my_chip = me // 4

    def fft_peer(step):
        k = (step + 1) // 2
        sign = 2 * (step % 2) - 1
        return lax.rem(me + sign * k + FFT, FFT)

    def ring_peer(step):
        past = step - 4
        away = jnp.where(step < 4, 0, past // 8 + 1)
        sign = 1 - 2 * (past % 2)
        turn = jnp.where(step < 4, step, jnp.where(step < 28, (past % 8) // 2, past % 4))
        chip = lax.rem(my_chip + sign * away + BAND, BAND)
        return chip * 4 + lax.rem(me + turn, 4)

    def rows_of(slot):
        return pl.ds(pl.multiple_of(slot * ROWS, ROWS), ROWS)

    def planes_of(device):
        return pl.ds(device * PLANES, PLANES)

    loads = [
        pltpu.make_async_copy(source, target, sem_in.at[k])
        for k, (source, target) in enumerate((
            (psi_hbm, psi),
            (pot_hbm, pot),
            (left_hbm, left_table),
            (right_hbm, right_table),
            (occ_hbm, occ),
        ))
    ]
    for load in loads:
        load.start()
    barrier = pltpu.get_barrier_semaphore()

    def sign_of(step):
        half = step // 2
        return FFT + (2 * (step % 2) - 1) * half

    @pl.loop(1, FFT)
    def _(step):
        pl.semaphore_signal(
            barrier,
            inc=1,
            device_id={"fft": lax.rem(me + FFT // 2 + sign_of(step), FFT)},
            device_id_type=MESH,
        )

    stands = jnp.logical_and(me >= 1, me < BAND)
    ahead = {"band": lax.rem(my_band + me, BAND)}
    behind = {"band": lax.rem(my_band - me + FFT, BAND)}

    @pl.when(stands)
    def _():
        pl.semaphore_signal(barrier, inc=1, device_id=ahead, device_id_type=MESH)

    for load in loads:
        load.wait()
    @pl.when(jnp.logical_not(stands))
    def _():
        pl.semaphore_wait(barrier, FFT - 1)

    @pl.when(stands)
    def _():
        pl.semaphore_wait(barrier, FFT)
        pl.semaphore_signal(sem_group_in, inc=1, device_id=behind, device_id_type=MESH)


    first_slot = lax.rem(my_band - me + FFT, BAND)
    for k in range(2):
        target = 2 * (first_slot + BAND * k) + (me // BAND) % 2

        @pl.when(target != me)
        def _():
            pltpu.make_async_remote_copy(
                src_ref=pot.at[:, rows_of(target // 2), :],
                dst_ref=col_pot.at[planes_of(me)],
                send_sem=send.at[1],
                recv_sem=sem_pot.at[0],
                device_id={"fft": target},
                device_id_type=MESH,
            ).start()

        @pl.when(target == me)
        def _():
            pltpu.make_async_copy(
                pot.at[:, rows_of(my_slot), :],
                col_pot.at[planes_of(me)],
                sem_pot.at[0],
            ).start()

    @pl.loop(1, FFT)
    def _(step):
        peer = ring_peer(step)
        pltpu.make_async_remote_copy(
            src_ref=psi.at[:, peer % 2, :, rows_of(peer // 2), :],
            dst_ref=col.at[pl.ds(0, 2), planes_of(me)],
            send_sem=send.at[0],
            recv_sem=sem_col,
            device_id={"fft": peer},
            device_id_type=MESH,
        ).start()

    pltpu.make_async_copy(
        psi.at[:, me % 2, :, rows_of(my_slot), :],
        col.at[pl.ds(0, 2), planes_of(me)],
        sem_col,
    ).start()

    left, right = left_table[...], right_table[...]

    for part_of in range(2):

        @pl.loop(0, 8, unroll=4)
        def _(index):
            band, plane = index // 4, index % 4
            tang[part_of, band, plane] = in_plane(left, right, psi[part_of, band, plane])

        @pl.loop(1, FFT)
        def _(step):
            peer = ring_peer(step)
            pltpu.make_async_remote_copy(
                src_ref=tang.at[part_of, peer % 2, :, rows_of(peer // 2), :],
                dst_ref=col.at[2 + part_of, planes_of(me)],
                send_sem=send.at[2],
                recv_sem=sem_tang.at[part_of],
                device_id={"fft": peer},
                device_id_type=MESH,
            ).start()

        pltpu.make_async_copy(
            tang.at[part_of, me % 2, :, rows_of(my_slot), :],
            col.at[2 + part_of, planes_of(me)],
            sem_tang.at[part_of],
        ).start()

    @pl.when(stands)
    def _():
        pl.semaphore_wait(sem_group_in, 1)
        pl.semaphore_signal(sem_groups_in, inc=1)

        @pl.loop(1, FFT)
        def _(step):
            pl.semaphore_signal(
                sem_groups_in,
                inc=1,
                device_id={"fft": lax.rem(me + step, FFT)},
                device_id_type=MESH,
            )

    pl.semaphore_wait(sem_groups_in, BAND - 1)

    wait_bytes(col_pot.at[pl.ds(0, 8)], sem_pot.at[0])
    first_device = lax.rem(my_band - my_slot + FFT, BAND) + BAND * (me % 2)

    @pl.loop(0, 2)
    def _(k):
        held = planes_of(first_device + 2 * BAND * k)

        @pl.loop(1, 2 * BAND)
        def _(step):
            seat = lax.rem(2 * my_band + me % 2 + step, 2 * BAND)
            pltpu.make_async_remote_copy(
                src_ref=col_pot.at[held],
                dst_ref=col_pot.at[held],
                send_sem=send.at[3],
                recv_sem=sem_pot.at[1],
                device_id={"fft": 2 * my_slot + seat % 2, "band": seat // 2},
                device_id_type=MESH,
            ).start()

    @pl.loop(0, 8, unroll=2)
    def _(index):
        band, plane = index // 4, index % 4
        values = pot[plane]
        real, imag = psi[0, band, plane], psi[1, band, plane]
        first_real = tang[0, band, plane] + values * real
        first_imag = tang[1, band, plane] + values * imag
        second_real = in_plane(left, right, first_real) + values * first_real
        second_imag = in_plane(left, right, first_imag) + values * first_imag
        local[0, band, plane] = real + TIME_STEP * first_imag - HALF_SQUARE * second_real
        local[1, band, plane] = imag - TIME_STEP * first_real - HALF_SQUARE * second_imag

    wait_bytes(col.at[pl.ds(0, 2)], sem_col)
    wait_bytes(col_pot.at[pl.ds(0, 120)], sem_pot.at[1])
    for part_of in range(2):
        sign = 1.0 - 2.0 * part_of
        wait_bytes(col.at[2 + part_of], sem_tang.at[part_of])

        for pair in range(0, ROWS, 2):

            def rows(ref, *index):
                return jnp.concatenate(
                    [ref[(*index, slice(None), pair + k)] for k in range(2)], axis=1
                )

            values = rows(col_pot)
            mine = rows(col, part_of)
            along = from_left(left, mine)
            inner = (
                (sign * TIME_STEP) * rows(col, 1 - part_of)
                - (2.0 * HALF_SQUARE) * rows(col, 2 + part_of)
                - HALF_SQUARE * (values * mine + along)
            )
            moved = from_left(left, inner) - HALF_SQUARE * (values * along)
            for k in range(2):
                back[part_of, :, pair + k, :] = moved[:, k * GRID : (k + 1) * GRID]

        @pl.loop(1, FFT)
        def _(step):
            peer = ring_peer(step)
            pltpu.make_async_remote_copy(
                src_ref=back.at[part_of, planes_of(peer)],
                dst_ref=ret.at[part_of, me % 2, :, rows_of(my_slot), :],
                send_sem=send.at[4],
                recv_sem=sem_ret if part_of == 0 else sem_group.at[my_chip],
                device_id={"fft": peer},
                device_id_type=MESH,
            ).start()

        pltpu.make_async_copy(
            back.at[part_of, planes_of(me)],
            ret.at[part_of, me % 2, :, rows_of(my_slot), :],
            sem_ret if part_of == 0 else sem_group.at[my_chip],
        ).start()

    wait_bytes(ret.at[0], sem_ret)

    @pl.loop(0, PLANES)
    def _(plane):
        low = local[0, 0, plane] + ret[0, 0, plane]
        high = local[0, 1, plane] + ret[0, 1, plane]
        local[0, 0, plane] = low
        local[0, 1, plane] = high
        part[plane] = occ[0] * (low * low) + occ[1] * (high * high)

    @pl.loop(0, BAND)
    def _(step):
        k = (step + 1) // 2
        sign = 2 * (step % 2) - 1
        block = lax.rem(my_chip + sign * k + BAND, BAND)
        rows = pl.ds(pl.multiple_of(block * OWN_ROWS, OWN_ROWS), OWN_ROWS)
        wait_bytes(ret.at[1, :, :, pl.ds(0, OWN_ROWS), :], sem_group.at[block])
        low = local[1, 0, :, rows, :] + ret[1, 0, :, rows, :]
        high = local[1, 1, :, rows, :] + ret[1, 1, :, rows, :]
        local[1, 0, :, rows, :] = low
        local[1, 1, :, rows, :] = high
        part[:, rows, :] = part[:, rows, :] + (occ[0] * (low * low) + occ[1] * (high * high))

        @pl.when(block != my_band)
        def _():
            pltpu.make_async_remote_copy(
                src_ref=part.at[:, rows, :],
                dst_ref=arrived.at[my_band],
                send_sem=send.at[5],
                recv_sem=sem_dens,
                device_id={"band": block},
                device_id_type=MESH,
            ).start()

        @pl.when(block == my_band)
        def _():
            pltpu.make_async_copy(part.at[:, rows, :], arrived.at[my_band], sem_dens).start()

    wait_bytes(arrived, sem_dens)
    total = arrived[0]
    for k in range(1, BAND):
        total = total + arrived[k]
    dens[...] = total
    rows_x[:, 8:24, :] = total
    edge_x[0] = dens[:, 14:16, :]
    edge_x[1] = dens[:, 0:2, :]

    halos = []
    for side in range(2):
        shift = 1 - 2 * side
        halos.append(
            pltpu.make_async_remote_copy(
                src_ref=dens.at[pl.ds(2 - 2 * side, 2)],
                dst_ref=halo_z.at[side],
                send_sem=send.at[6 + side],
                recv_sem=sem_halo.at[side],
                device_id={"fft": lax.rem(me + shift + FFT, FFT)},
                device_id_type=MESH,
            )
        )
        halos.append(
            pltpu.make_async_remote_copy(
                src_ref=edge_x.at[side],
                dst_ref=halo_x.at[side],
                send_sem=send.at[8 + side],
                recv_sem=sem_halo.at[2 + side],
                device_id={"band": lax.rem(my_band + shift + BAND, BAND)},
                device_id_type=MESH,
            )
        )
    for halo in halos:
        halo.start()

    scale = 1.0 / (12.0 * SPACING)
    grad_y = (
        8.0 * (pltpu.roll(total, GRID - 1, 2) - pltpu.roll(total, 1, 2))
        - (pltpu.roll(total, GRID - 2, 2) - pltpu.roll(total, 2, 2))
    ) * scale

    wait_bytes(col.at[pl.ds(0, 2), pl.ds(0, 124)], send.at[0])
    wait_bytes(col.at[pl.ds(0, 2), pl.ds(0, 124)], send.at[2])
    wait_bytes(back.at[:, pl.ds(0, 124)], send.at[4])
    wait_bytes(col_pot.at[pl.ds(0, 120)], send.at[3])
    wait_bytes(arrived.at[pl.ds(0, 7)], send.at[5])
    holds_own = jnp.logical_and(
        lax.rem(me + my_slot - my_band + FFT, BAND) == 0, me % 2 == (me // BAND) % 2
    )

    @pl.when(holds_own)
    def _():
        wait_bytes(col_pot.at[pl.ds(0, 4)], send.at[1])

    @pl.when(jnp.logical_not(holds_own))
    def _():
        wait_bytes(col_pot.at[pl.ds(0, 8)], send.at[1])

    for halo in halos:
        halo.wait()
    rows_x[:, 6:8, :] = halo_x[0]
    rows_x[:, 24:26, :] = halo_x[1]
    grad_x = (
        8.0 * (rows_x[:, 9:25, :] - rows_x[:, 7:23, :])
        - (rows_x[:, 10:26, :] - rows_x[:, 6:22, :])
    ) * scale
    stack = jnp.concatenate([halo_z[0], total, halo_z[1]], axis=0)
    grad_z = (8.0 * (stack[3:7] - stack[1:5]) - (stack[4:8] - stack[0:4])) * scale
    summed_ref[0] = grad_z * grad_z + grad_x * grad_x + grad_y * grad_y
    summed_ref[1] = total


def exchange_terms(square, density):
    power = jnp.exp((4.0 / 3.0) * jnp.log(density))
    reduced = jnp.sqrt(square) / (FERMI_FACTOR * power)
    enhance = 1.0 + KAPPA_PBE - KAPPA_PBE / (1.0 + MU_PBE * reduced * reduced / KAPPA_PBE)
    return reduced, -SLATER_FACTOR * power * enhance


def finish(moved, summed, moved_out, reduced_out, energy_out, terms, sem_out):
    stores = [
        pltpu.make_async_copy(moved.at[k // 2, k % 2], moved_out.at[k // 2, k % 2], sem_out.at[k])
        for k in range(4)
    ]
    stores.append(pltpu.make_async_copy(terms.at[0], reduced_out, sem_out.at[4]))
    stores.append(pltpu.make_async_copy(terms.at[1], energy_out, sem_out.at[5]))
    for store in stores[:4]:
        store.start()
    terms[0], terms[1] = exchange_terms(summed[0], summed[1])
    for store in stores[4:]:
        store.start()
    for store in stores:
        store.wait()


def per_device(wavefunctions, potential, occupation):
    in_hbm = pl.BlockSpec(memory_space=pltpu.HBM)
    vmem = pl.BlockSpec(memory_space=pltpu.VMEM)
    block = (PLANES, OWN_ROWS, GRID)
    planes = (2, 2, PLANES, GRID, GRID)
    dma = pltpu.SemaphoreType.DMA
    moved, summed = pl.pallas_call(
        kernel,
        name="taylor_step",
        out_shape=(
            pltpu.VMEM(planes, F32),
            pltpu.VMEM((2, *block), F32),
        ),
        in_specs=[in_hbm] * 5,
        out_specs=(vmem, vmem),
        scratch_shapes=[
            pltpu.SMEM((2,), F32),
            pltpu.VMEM(planes, F32),
            pltpu.VMEM((PLANES, GRID, GRID), F32),
            pltpu.VMEM((GRID, 3 * GRID), BF16),
            pltpu.VMEM((3 * GRID, GRID), BF16),
            pltpu.VMEM(planes, F32),
            pltpu.VMEM((4, GRID, ROWS, GRID), F32),
            pltpu.VMEM((GRID, ROWS, GRID), F32),
            pltpu.VMEM((2, GRID, ROWS, GRID), F32),
            pltpu.VMEM(planes, F32),
            pltpu.VMEM((PLANES, GRID, GRID), F32),
            pltpu.VMEM((BAND, *block), F32),
            pltpu.VMEM(block, F32),
            pltpu.VMEM((2, 2, OWN_ROWS, GRID), F32),
            pltpu.VMEM((2, PLANES, 2, GRID), F32),
            pltpu.VMEM((2, PLANES, 2, GRID), F32),
            pltpu.VMEM((PLANES, 32, GRID), F32),
            dma((5,)),
            dma,
            dma((2,)),
            dma,
            dma((BAND,)),
            dma((2,)),
            dma,
            dma((4,)),
            dma((10,)),
            pltpu.SemaphoreType.REGULAR,
            pltpu.SemaphoreType.REGULAR,
        ],
        compiler_params=pltpu.CompilerParams(
            collective_id=0, has_side_effects=True, vmem_limit_bytes=62000000
        ),
    )(occupation, wavefunctions, potential, *kinetic_parts())
    return pl.pallas_call(
        finish,
        name="exchange",
        out_shape=(
            jax.ShapeDtypeStruct(planes, F32),
            jax.ShapeDtypeStruct(block, F32),
            jax.ShapeDtypeStruct(block, F32),
        ),
        in_specs=[vmem, vmem],
        out_specs=(in_hbm, in_hbm, in_hbm),
        scratch_shapes=[
            pltpu.VMEM((2, *block), F32),
            dma((6,)),
        ],
        compiler_params=pltpu.CompilerParams(vmem_limit_bytes=16000000),
    )(moved, summed)


def solution(mesh):
    in_specs = (P(None, "band", "fft", None, None), P("fft", None, None), P("band"))
    out_specs = (P(None, "band", "fft", None, None), P("fft", "band", None), P("fft", "band", None))
    return jax.shard_map(
        per_device, mesh=mesh, in_specs=in_specs, out_specs=out_specs, check_vma=False
    )
```

```python
import functools
import math

import jax
import jax.numpy as jnp
import numpy as np
from jax import lax
from jax.experimental import pallas as pl
from jax.experimental.pallas import tpu as pltpu
from jax.sharding import PartitionSpec as P

SPACING = 0.4
TIME_STEP = 0.012
HALF_SQUARE = 0.5 * TIME_STEP * TIME_STEP
KAPPA_PBE = 0.804
MU_PBE = 0.21951
FERMI_FACTOR = 2.0 * math.pow(3.0 * math.pi * math.pi, 1.0 / 3.0)
SLATER_FACTOR = 0.75 * math.pow(3.0 / math.pi, 1.0 / 3.0)

GRID = 128
FFT = 32
BAND = 8
PLANES = GRID // FFT
ROWS = 8
OWN_ROWS = GRID // BAND
MESH = pl.DeviceIdType.MESH
F32 = jnp.float32
BF16 = jnp.bfloat16


def kinetic_matrix():
    counter = np.arange(GRID)
    signed = np.where(counter < GRID // 2, counter, counter - GRID)
    half_squares = 0.5 * (2.0 * np.pi * signed / (GRID * SPACING)) ** 2
    phase = np.outer(counter, counter) % GRID
    column = np.cos(2.0 * np.pi * phase / GRID) @ half_squares / GRID
    return column[(counter[:, None] - counter[None, :]) % GRID]


def kinetic_parts():
    matrix = kinetic_matrix()
    high = matrix.astype(jnp.bfloat16)
    low = (matrix - high.astype(np.float64)).astype(jnp.bfloat16)
    beside = np.concatenate([high, high, low], axis=1)
    return beside, beside.T.copy()


def split(values):
    high = values.astype(BF16)
    return high, (values - high.astype(F32)).astype(BF16)


def dot(a, b):
    return jnp.dot(a, b, preferred_element_type=F32)


def from_left(left, values):
    high, low = split(values)
    return dot(left, jnp.concatenate([high, low, high], axis=0))


def in_plane(left, right, values):
    high, low = split(values)
    return dot(left, jnp.concatenate([high, low, high], axis=0)) + dot(
        jnp.concatenate([high, low, high], axis=1), right
    )


def wait_bytes(ref, sem):
    pltpu.make_async_copy(ref, ref, sem).wait()


def kernel(
    occ_hbm,
    psi_hbm,
    pot_hbm,
    left_hbm,
    right_hbm,
    local,
    summed_ref,
    occ,
    psi,
    pot,
    left_table,
    right_table,
    tang,
    col,
    col_pot,
    back,
    ret,
    part,
    arrived,
    dens,
    halo_z,
    edge_x,
    halo_x,
    rows_x,
    sem_in,
    sem_col,
    sem_tang,
    sem_ret,
    sem_group,
    sem_pot,
    sem_dens,
    sem_halo,
    send,
    sem_group_in,
    sem_groups_in,
):
    me = lax.axis_index("fft")
    my_band = lax.axis_index("band")
    my_slot = me // 2
    my_chip = me // 4

    def fft_peer(step):
        k = (step + 1) // 2
        sign = 2 * (step % 2) - 1
        return lax.rem(me + sign * k + FFT, FFT)

    def ring_peer(step):
        past = step - 4
        away = jnp.where(step < 4, 0, past // 8 + 1)
        sign = 1 - 2 * (past % 2)
        turn = jnp.where(step < 4, step, jnp.where(step < 28, (past % 8) // 2, past % 4))
        chip = lax.rem(my_chip + sign * away + BAND, BAND)
        return chip * 4 + lax.rem(me + turn, 4)

    def rows_of(slot):
        return pl.ds(pl.multiple_of(slot * ROWS, ROWS), ROWS)

    def planes_of(device):
        return pl.ds(device * PLANES, PLANES)

    loads = [
        pltpu.make_async_copy(source, target, sem_in.at[k])
        for k, (source, target) in enumerate((
            (psi_hbm, psi),
            (pot_hbm, pot),
            (left_hbm, left_table),
            (right_hbm, right_table),
            (occ_hbm, occ),
        ))
    ]
    for load in loads:
        load.start()
    barrier = pltpu.get_barrier_semaphore()

    def sign_of(step):
        half = step // 2
        return FFT + (2 * (step % 2) - 1) * half

    @pl.loop(1, FFT)
    def _(step):
        pl.semaphore_signal(
            barrier,
            inc=1,
            device_id={"fft": lax.rem(me + FFT // 2 + sign_of(step), FFT)},
            device_id_type=MESH,
        )

    stands = jnp.logical_and(me >= 1, me < BAND)
    ahead = {"band": lax.rem(my_band + me, BAND)}
    behind = {"band": lax.rem(my_band - me + FFT, BAND)}

    @pl.when(stands)
    def _():
        pl.semaphore_signal(barrier, inc=1, device_id=ahead, device_id_type=MESH)

    for load in loads:
        load.wait()
    @pl.when(jnp.logical_not(stands))
    def _():
        pl.semaphore_wait(barrier, FFT - 1)

    @pl.when(stands)
    def _():
        pl.semaphore_wait(barrier, FFT)
        pl.semaphore_signal(sem_group_in, inc=1, device_id=behind, device_id_type=MESH)


    first_slot = lax.rem(my_band - me + FFT, BAND)
    for k in range(2):
        target = 2 * (first_slot + BAND * k) + (me // BAND) % 2

        @pl.when(target != me)
        def _():
            pltpu.make_async_remote_copy(
                src_ref=pot.at[:, rows_of(target // 2), :],
                dst_ref=col_pot.at[planes_of(me)],
                send_sem=send.at[1],
                recv_sem=sem_pot.at[0],
                device_id={"fft": target},
                device_id_type=MESH,
            ).start()

        @pl.when(target == me)
        def _():
            pltpu.make_async_copy(
                pot.at[:, rows_of(my_slot), :],
                col_pot.at[planes_of(me)],
                sem_pot.at[0],
            ).start()

    @pl.loop(1, FFT)
    def _(step):
        peer = ring_peer(step)
        pltpu.make_async_remote_copy(
            src_ref=psi.at[:, peer % 2, :, rows_of(peer // 2), :],
            dst_ref=col.at[pl.ds(0, 2), planes_of(me)],
            send_sem=send.at[0],
            recv_sem=sem_col,
            device_id={"fft": peer},
            device_id_type=MESH,
        ).start()

    pltpu.make_async_copy(
        psi.at[:, me % 2, :, rows_of(my_slot), :],
        col.at[pl.ds(0, 2), planes_of(me)],
        sem_col,
    ).start()

    left, right = left_table[...], right_table[...]

    for part_of in range(2):

        @pl.loop(0, 8, unroll=4)
        def _(index):
            band, plane = index // 4, index % 4
            tang[part_of, band, plane] = in_plane(left, right, psi[part_of, band, plane])

        @pl.loop(1, FFT)
        def _(step):
            peer = ring_peer(step)
            pltpu.make_async_remote_copy(
                src_ref=tang.at[part_of, peer % 2, :, rows_of(peer // 2), :],
                dst_ref=col.at[2 + part_of, planes_of(me)],
                send_sem=send.at[2],
                recv_sem=sem_tang.at[part_of],
                device_id={"fft": peer},
                device_id_type=MESH,
            ).start()

        pltpu.make_async_copy(
            tang.at[part_of, me % 2, :, rows_of(my_slot), :],
            col.at[2 + part_of, planes_of(me)],
            sem_tang.at[part_of],
        ).start()

    @pl.when(stands)
    def _():
        pl.semaphore_wait(sem_group_in, 1)
        pl.semaphore_signal(sem_groups_in, inc=1)

        @pl.loop(1, FFT)
        def _(step):
            pl.semaphore_signal(
                sem_groups_in,
                inc=1,
                device_id={"fft": lax.rem(me + step, FFT)},
                device_id_type=MESH,
            )

    pl.semaphore_wait(sem_groups_in, BAND - 1)

    wait_bytes(col_pot.at[pl.ds(0, 8)], sem_pot.at[0])
    first_device = lax.rem(my_band - my_slot + FFT, BAND) + BAND * (me % 2)

    @pl.loop(0, 2)
    def _(k):
        held = planes_of(first_device + 2 * BAND * k)

        @pl.loop(1, 2 * BAND)
        def _(step):
            seat = lax.rem(2 * my_band + me % 2 + step, 2 * BAND)
            pltpu.make_async_remote_copy(
                src_ref=col_pot.at[held],
                dst_ref=col_pot.at[held],
                send_sem=send.at[3],
                recv_sem=sem_pot.at[1],
                device_id={"fft": 2 * my_slot + seat % 2, "band": seat // 2},
                device_id_type=MESH,
            ).start()

    @pl.loop(0, 8, unroll=2)
    def _(index):
        band, plane = index // 4, index % 4
        values = pot[plane]
        real, imag = psi[0, band, plane], psi[1, band, plane]
        first_real = tang[0, band, plane] + values * real
        first_imag = tang[1, band, plane] + values * imag
        second_real = in_plane(left, right, first_real) + values * first_real
        second_imag = in_plane(left, right, first_imag) + values * first_imag
        local[0, band, plane] = real + TIME_STEP * first_imag - HALF_SQUARE * second_real
        local[1, band, plane] = imag - TIME_STEP * first_real - HALF_SQUARE * second_imag

    wait_bytes(col.at[pl.ds(0, 2)], sem_col)
    wait_bytes(col_pot.at[pl.ds(0, 120)], sem_pot.at[1])
    for part_of in range(2):
        sign = 1.0 - 2.0 * part_of
        wait_bytes(col.at[2 + part_of], sem_tang.at[part_of])

        for pair in range(0, ROWS, 2):

            def rows(ref, *index):
                return jnp.concatenate(
                    [ref[(*index, slice(None), pair + k)] for k in range(2)], axis=1
                )

            values = rows(col_pot)
            mine = rows(col, part_of)
            along = from_left(left, mine)
            inner = (
                (sign * TIME_STEP) * rows(col, 1 - part_of)
                - (2.0 * HALF_SQUARE) * rows(col, 2 + part_of)
                - HALF_SQUARE * (values * mine + along)
            )
            moved = from_left(left, inner) - HALF_SQUARE * (values * along)
            for k in range(2):
                back[part_of, :, pair + k, :] = moved[:, k * GRID : (k + 1) * GRID]

        @pl.loop(1, FFT)
        def _(step):
            peer = ring_peer(step)
            pltpu.make_async_remote_copy(
                src_ref=back.at[part_of, planes_of(peer)],
                dst_ref=ret.at[part_of, me % 2, :, rows_of(my_slot), :],
                send_sem=send.at[4],
                recv_sem=sem_ret if part_of == 0 else sem_group.at[my_chip],
                device_id={"fft": peer},
                device_id_type=MESH,
            ).start()

        pltpu.make_async_copy(
            back.at[part_of, planes_of(me)],
            ret.at[part_of, me % 2, :, rows_of(my_slot), :],
            sem_ret if part_of == 0 else sem_group.at[my_chip],
        ).start()

    wait_bytes(ret.at[0], sem_ret)

    @pl.loop(0, PLANES)
    def _(plane):
        low = local[0, 0, plane] + ret[0, 0, plane]
        high = local[0, 1, plane] + ret[0, 1, plane]
        local[0, 0, plane] = low
        local[0, 1, plane] = high
        part[plane] = occ[0] * (low * low) + occ[1] * (high * high)

    @pl.loop(0, BAND)
    def _(step):
        k = (step + 1) // 2
        sign = 2 * (step % 2) - 1
        block = lax.rem(my_chip + sign * k + BAND, BAND)
        rows = pl.ds(pl.multiple_of(block * OWN_ROWS, OWN_ROWS), OWN_ROWS)
        wait_bytes(ret.at[1, :, :, pl.ds(0, OWN_ROWS), :], sem_group.at[block])
        low = local[1, 0, :, rows, :] + ret[1, 0, :, rows, :]
        high = local[1, 1, :, rows, :] + ret[1, 1, :, rows, :]
        local[1, 0, :, rows, :] = low
        local[1, 1, :, rows, :] = high
        part[:, rows, :] = part[:, rows, :] + (occ[0] * (low * low) + occ[1] * (high * high))

        @pl.when(block != my_band)
        def _():
            pltpu.make_async_remote_copy(
                src_ref=part.at[:, rows, :],
                dst_ref=arrived.at[my_band],
                send_sem=send.at[5],
                recv_sem=sem_dens,
                device_id={"band": block},
                device_id_type=MESH,
            ).start()

        @pl.when(block == my_band)
        def _():
            pltpu.make_async_copy(part.at[:, rows, :], arrived.at[my_band], sem_dens).start()

    wait_bytes(arrived, sem_dens)
    total = arrived[0]
    for k in range(1, BAND):
        total = total + arrived[k]
    dens[...] = total
    rows_x[:, 8:24, :] = total
    edge_x[0] = dens[:, 14:16, :]
    edge_x[1] = dens[:, 0:2, :]

    halos = []
    for side in range(2):
        shift = 1 - 2 * side
        halos.append(
            pltpu.make_async_remote_copy(
                src_ref=dens.at[pl.ds(2 - 2 * side, 2)],
                dst_ref=halo_z.at[side],
                send_sem=send.at[6 + side],
                recv_sem=sem_halo.at[side],
                device_id={"fft": lax.rem(me + shift + FFT, FFT)},
                device_id_type=MESH,
            )
        )
        halos.append(
            pltpu.make_async_remote_copy(
                src_ref=edge_x.at[side],
                dst_ref=halo_x.at[side],
                send_sem=send.at[8 + side],
                recv_sem=sem_halo.at[2 + side],
                device_id={"band": lax.rem(my_band + shift + BAND, BAND)},
                device_id_type=MESH,
            )
        )
    for halo in halos:
        halo.start()

    scale = 1.0 / (12.0 * SPACING)
    grad_y = (
        8.0 * (pltpu.roll(total, GRID - 1, 2) - pltpu.roll(total, 1, 2))
        - (pltpu.roll(total, GRID - 2, 2) - pltpu.roll(total, 2, 2))
    ) * scale

    for halo in halos:
        halo.wait()
    rows_x[:, 6:8, :] = halo_x[0]
    rows_x[:, 24:26, :] = halo_x[1]
    grad_x = (
        8.0 * (rows_x[:, 9:25, :] - rows_x[:, 7:23, :])
        - (rows_x[:, 10:26, :] - rows_x[:, 6:22, :])
    ) * scale
    stack = jnp.concatenate([halo_z[0], total, halo_z[1]], axis=0)
    grad_z = (8.0 * (stack[3:7] - stack[1:5]) - (stack[4:8] - stack[0:4])) * scale
    summed_ref[0] = grad_z * grad_z + grad_x * grad_x + grad_y * grad_y
    summed_ref[1] = total

    wait_bytes(col.at[pl.ds(0, 2), pl.ds(0, 124)], send.at[0])
    wait_bytes(col.at[pl.ds(0, 2), pl.ds(0, 124)], send.at[2])
    wait_bytes(back.at[:, pl.ds(0, 124)], send.at[4])
    wait_bytes(col_pot.at[pl.ds(0, 120)], send.at[3])
    wait_bytes(arrived.at[pl.ds(0, 7)], send.at[5])
    holds_own = jnp.logical_and(
        lax.rem(me + my_slot - my_band + FFT, BAND) == 0, me % 2 == (me // BAND) % 2
    )

    @pl.when(holds_own)
    def _():
        wait_bytes(col_pot.at[pl.ds(0, 4)], send.at[1])

    @pl.when(jnp.logical_not(holds_own))
    def _():
        wait_bytes(col_pot.at[pl.ds(0, 8)], send.at[1])


def exchange_terms(square, density):
    power = jnp.exp((4.0 / 3.0) * jnp.log(density))
    reduced = jnp.sqrt(square) / (FERMI_FACTOR * power)
    enhance = 1.0 + KAPPA_PBE - KAPPA_PBE / (1.0 + MU_PBE * reduced * reduced / KAPPA_PBE)
    return reduced, -SLATER_FACTOR * power * enhance


def finish(moved, summed, moved_out, reduced_out, energy_out, terms, sem_out):
    stores = [
        pltpu.make_async_copy(moved.at[k // 2, k % 2], moved_out.at[k // 2, k % 2], sem_out.at[k])
        for k in range(4)
    ]
    stores.append(pltpu.make_async_copy(terms.at[0], reduced_out, sem_out.at[4]))
    stores.append(pltpu.make_async_copy(terms.at[1], energy_out, sem_out.at[5]))
    for store in stores[:4]:
        store.start()
    terms[0], terms[1] = exchange_terms(summed[0], summed[1])
    for store in stores[4:]:
        store.start()
    for store in stores:
        store.wait()


def per_device(wavefunctions, potential, occupation):
    in_hbm = pl.BlockSpec(memory_space=pltpu.HBM)
    vmem = pl.BlockSpec(memory_space=pltpu.VMEM)
    block = (PLANES, OWN_ROWS, GRID)
    planes = (2, 2, PLANES, GRID, GRID)
    dma = pltpu.SemaphoreType.DMA
    moved, summed = pl.pallas_call(
        kernel,
        name="taylor_step",
        out_shape=(
            pltpu.VMEM(planes, F32),
            pltpu.VMEM((2, *block), F32),
        ),
        in_specs=[in_hbm] * 5,
        out_specs=(vmem, vmem),
        scratch_shapes=[
            pltpu.SMEM((2,), F32),
            pltpu.VMEM(planes, F32),
            pltpu.VMEM((PLANES, GRID, GRID), F32),
            pltpu.VMEM((GRID, 3 * GRID), BF16),
            pltpu.VMEM((3 * GRID, GRID), BF16),
            pltpu.VMEM(planes, F32),
            pltpu.VMEM((4, GRID, ROWS, GRID), F32),
            pltpu.VMEM((GRID, ROWS, GRID), F32),
            pltpu.VMEM((2, GRID, ROWS, GRID), F32),
            pltpu.VMEM(planes, F32),
            pltpu.VMEM((PLANES, GRID, GRID), F32),
            pltpu.VMEM((BAND, *block), F32),
            pltpu.VMEM(block, F32),
            pltpu.VMEM((2, 2, OWN_ROWS, GRID), F32),
            pltpu.VMEM((2, PLANES, 2, GRID), F32),
            pltpu.VMEM((2, PLANES, 2, GRID), F32),
            pltpu.VMEM((PLANES, 32, GRID), F32),
            dma((5,)),
            dma,
            dma((2,)),
            dma,
            dma((BAND,)),
            dma((2,)),
            dma,
            dma((4,)),
            dma((10,)),
            pltpu.SemaphoreType.REGULAR,
            pltpu.SemaphoreType.REGULAR,
        ],
        compiler_params=pltpu.CompilerParams(
            collective_id=0, has_side_effects=True, vmem_limit_bytes=62000000
        ),
    )(occupation, wavefunctions, potential, *kinetic_parts())
    return pl.pallas_call(
        finish,
        name="exchange",
        out_shape=(
            jax.ShapeDtypeStruct(planes, F32),
            jax.ShapeDtypeStruct(block, F32),
            jax.ShapeDtypeStruct(block, F32),
        ),
        in_specs=[vmem, vmem],
        out_specs=(in_hbm, in_hbm, in_hbm),
        scratch_shapes=[
            pltpu.VMEM((2, *block), F32),
            dma((6,)),
        ],
        compiler_params=pltpu.CompilerParams(vmem_limit_bytes=16000000),
    )(moved, summed)


def solution(mesh):
    in_specs = (P(None, "band", "fft", None, None), P("fft", None, None), P("band"))
    out_specs = (P(None, "band", "fft", None, None), P("fft", "band", None), P("fft", "band", None))
    return jax.shard_map(
        per_device, mesh=mesh, in_specs=in_specs, out_specs=out_specs, check_vma=False
    )
```
